256 devices in a mesh: gx: 32 (over z, x_lo, core), gy: 8 (over x_hi, y).
Axes of the slice: x: 4 (x_hi: 2, x_lo: 2; x = x_hi * 2 + x_lo), y: 4, z: 8, core: 2. Of those that a mesh axis runs over, the one named last changes fastest.
Arguments:
- volt: float32 [256, 512, 2048], P('gx', 'gy'), may hold values from -6 to 6
- drive: float32 [256, 512, 2048], P('gx', 'gy'), may hold values from -6 to 6
- region: int32 [256, 512, 32], P('gx', 'gy'), may hold values from 0 to 7
- diode_mask: int32 [256, 512, 32], P('gx', 'gy'), may hold values 0 or 1
- sigma_table: float32 [8], replicated, may hold values from 0.3 to 3
- cap_table: float32 [8], replicated, may hold values from 0.1 to 1
Outputs:
- residual: float32 [256, 512, 2048], P('gx', 'gy')
- coef_norms: float32 [64], replicated
The draws below stay inside these ranges and needn't reach their ends.
All inputs are finite; a program needn't handle non-finite values. No bound on the sum of `diode_mask` on one device may be relied on, other than what follows from the above.
Results may differ from the reference program's by a relative error of at most 0.0003.
Values sent between devices are 32-bit elements; how exact they have to be, the bound alone decides.
A program may use at most 192 MiB of HBM per device.

```python
import math
import jax
import jax.numpy as jnp
from jax import lax

NZ = 32
H = 32
KC = 64
S = 256
REGIONS = 8
NX = 256
NY = 512


def with_ends(values, key, least, high):
    extent = values.shape
    place = [jax.random.randint(jax.random.fold_in(key, axis), (), 0, extent[axis]) for axis in range(len(extent))]
    values = values.at[tuple(place)].set(least)
    longest = extent.index(max(extent))
    place[longest] = (place[longest] + 1) % extent[longest]
    return values.at[tuple(place)].set(high)


def shard_levels(rng, shape, shards, least, high):
    def one(dim, shards_of):
        draws = jax.random.uniform(jax.random.fold_in(jax.random.fold_in(rng, 6), dim), (shards_of,), jnp.float32, least / len(shards), high / len(shards))
        return jnp.repeat(jnp.exp(draws), shape[dim] // shards_of).reshape((-1,) + (1,) * (len(shape) - dim - 1))

    loudness = one(*shards[0])
    for cut in shards[1:]:
        loudness = loudness * one(*cut)
    return loudness


def noise(stream_key, shape, spread, bound, pieces=(), held_as=jnp.bfloat16):
    gain = shard_levels(stream_key, shape, pieces, -0.22, 0.18) if pieces else 1.0
    entries = jax.random.normal(stream_key, shape, jnp.float32) * spread * gain
    return jnp.minimum(jnp.maximum(entries, -bound), bound).astype(held_as)


def setup_inputs(seed: int = 0) -> dict:
    key_of = jax.random.split(jax.random.key(seed), 7)
    return {
        "volt": noise(key_of[0], (NX, NY, NZ * KC), 1.0, 6.0, ((0, 32), (1, 8)), jnp.float32),
        "drive": noise(key_of[1], (NX, NY, NZ * KC), 1.0, 6.0, ((0, 32), (1, 8)), jnp.float32),
        "region": with_ends(jax.random.randint(key_of[2], (NX, NY, NZ), 0, REGIONS), jax.random.fold_in(key_of[2], 1), 0, REGIONS - 1).astype(jnp.int32),
        "diode_mask": with_ends((jax.random.randint(key_of[3], (NX, NY, NZ), 0, 4) < 1).astype(jnp.int32), jax.random.fold_in(key_of[3], 1), 0, 1),
        "sigma_table": jnp.clip(jnp.exp(jax.random.uniform(key_of[4], (REGIONS,), jnp.float32, math.log(0.3), math.log(3.0))), 0.3, 3.0),
        "cap_table": jnp.clip(jnp.exp(jax.random.uniform(key_of[5], (REGIONS,), jnp.float32, math.log(0.1), math.log(1.0))), 0.1, 1.0),
    }


base_freq = 0.1
norm_eps = 1e-06

def cut_slab(array, first_idx, last_idx, along):
    return lax.slice_in_dim(array, first_idx, last_idx, axis=along)

def harmonic_mean(left, right):
    return 2.0 * left * right / (left + right)

def open_terms(volt_field, conduct, along):
    cell_count = volt_field.shape[along]
    widths = [(0, 0)] * volt_field.ndim
    widths[along] = (1, 1)
    padded_volt = jnp.pad(volt_field, widths)
    padded_cond = jnp.pad(conduct, widths)
    face_flux = harmonic_mean(cut_slab(padded_cond, 0, cell_count + 1, along), cut_slab(padded_cond, 1, cell_count + 2, along)) * (cut_slab(padded_volt, 1, cell_count + 2, along) - cut_slab(padded_volt, 0, cell_count + 1, along))
    return cut_slab(face_flux, 0, cell_count, along) - cut_slab(face_flux, 1, cell_count + 1, along)

def time_derivative(coefs):
    half_count = coefs.shape[-1] // 2
    orders = base_freq * jnp.arange(1, half_count + 1, dtype=jnp.float32)
    return jnp.concatenate([orders * coefs[..., half_count:], -orders * coefs[..., :half_count]], axis=-1)

def spectral_tables(harmonics, samples):
    orders = jnp.arange(1, harmonics + 1, dtype=jnp.float32)
    times = 2.0 * math.pi * jnp.arange(samples, dtype=jnp.float32) / samples
    angles = orders[:, None] * times[None, :]
    synthesis = jnp.concatenate([jnp.cos(angles), jnp.sin(angles)], axis=0)
    analysis = synthesis.T * (2.0 / samples)
    return (synthesis, analysis)

def nonlinear_row(volt_row, diode_row, synthesis, analysis):
    coef_count = volt_row.shape[-1]
    flat = volt_row.reshape(-1, coef_count)
    cell_count = flat.shape[0]
    samples = jnp.dot(flat, synthesis, precision=lax.Precision.HIGHEST, preferred_element_type=jnp.float32)
    current = jax.nn.softplus(2.0 * samples) * 0.5
    charge = jnp.tanh(samples) * 0.5
    projected = jnp.dot(jnp.concatenate([current, charge], axis=0), analysis, precision=lax.Precision.HIGHEST, preferred_element_type=jnp.float32)
    combined = projected[:cell_count] + time_derivative(projected[cell_count:])
    return combined.reshape(volt_row.shape) * diode_row[..., None]

def reference(volt, drive, region, diode_mask, sigma_table, cap_table):
    conduct = jnp.take(sigma_table, region)[..., None]
    capacity = jnp.take(cap_table, region)[..., None]
    volt_field = volt.reshape(NX, NY, NZ, KC)
    drive_field = drive.reshape(NX, NY, NZ, KC)
    diode_field = diode_mask.astype(jnp.float32)
    synthesis, analysis = spectral_tables(H, S)

    def picker(array, row_index):
        return lax.dynamic_index_in_dim(array, row_index, 0, keepdims=False)

    def one_row(row_index):
        prev_row = (row_index - 1 + NX) % NX
        next_row = (row_index + 1) % NX
        volt_here = picker(volt_field, row_index)
        cond_here = picker(conduct, row_index)
        volt_prev = picker(volt_field, prev_row)
        cond_prev = picker(conduct, prev_row)
        volt_next = picker(volt_field, next_row)
        cond_next = picker(conduct, next_row)
        below_flux = harmonic_mean(cond_prev, cond_here) * (volt_here - volt_prev)
        above_flux = harmonic_mean(cond_here, cond_next) * (volt_next - volt_here)
        row_terms = below_flux - above_flux
        col_terms = open_terms(volt_here, cond_here, 0)
        depth_terms = open_terms(volt_here, cond_here, 1)
        diode_part = nonlinear_row(volt_here, picker(diode_field, row_index), synthesis, analysis)
        residual = row_terms + col_terms + depth_terms + picker(capacity, row_index) * time_derivative(volt_here) + diode_part - picker(drive_field, row_index)
        return (residual, lax.optimization_barrier(jnp.sum(residual * residual, axis=(0, 1))))
    residual, row_squares = lax.map(one_row, jnp.arange(NX, dtype=jnp.int32))
    summed = lax.optimization_barrier(jnp.sum(row_squares, axis=0))
    norms_out = jnp.sqrt(summed / (NX * NY * NZ) + norm_eps)
    return (residual.reshape(NX, NY, NZ * KC), norms_out)
```

```python
import functools
import math

import jax
import jax.numpy as jnp
import numpy as np
from jax import lax
from jax.experimental import pallas as pl
from jax.experimental.pallas import tpu as pltpu
from jax.sharding import PartitionSpec as P

NZ = 32
H = 32
KC = 64
S = 256
REGIONS = 8
BASE_FREQ = 0.1
NORM_EPS = 1e-06
LANES = 128
ZT = NZ * KC // LANES
PAD = 8
CHUNKS = 4

MESH = pl.DeviceIdType.MESH
F32 = jnp.float32
BF16 = jnp.bfloat16


def split(table):
    high = table.astype(jnp.bfloat16)
    low = (table - high.astype(np.float64)).astype(jnp.bfloat16)
    return high, low


def spectral_tables():
    orders = np.arange(1, H + 1, dtype=np.float64)
    steps = np.arange(S, dtype=np.int64)
    angles = 2.0 * math.pi * ((orders[:, None].astype(np.int64) * steps[None, :]) % S) / S
    cosines, sines = np.cos(angles), np.sin(angles)
    synthesis = np.concatenate([cosines, sines], axis=0)
    analysis = synthesis.T * (2.0 / S)
    freq = BASE_FREQ * orders
    derived = np.concatenate([freq * analysis[:, H:], -freq * analysis[:, :H]], axis=1)
    high, low = split(synthesis)
    ws = np.concatenate([high, high, low, low], axis=0)
    both = np.concatenate([analysis, derived], axis=0)
    high, low = split(both)
    wa = np.zeros((2, 2 * S, 2, LANES), jnp.bfloat16)
    for half in range(2):
        wa[half, :, 0, half * KC : half * KC + KC] = high
        wa[half, :, 1, half * KC : half * KC + KC] = low
    return ws, wa.reshape(4 * S, 2 * LANES)


def harmonic_mean(left, right):
    return 2.0 * left * right / (left + right)


def pick(region, table):
    value = jnp.full(region.shape, table[0], F32)
    for idx in range(1, REGIONS):
        value = jnp.where(region == idx, table[idx], value)
    return value


def widen(compact):
    rows, count = compact.shape
    return jnp.concatenate([compact, jnp.zeros((rows, LANES - count), compact.dtype)], axis=1)


def spread(compact, index):
    return jnp.take_along_axis(compact, index, axis=1, mode="promise_in_bounds")


def kernel(
    nx, ny, rows, cols, cells,
    volt, drive, region, mask, sigma, cap, ws_hbm, wa_hbm,
    out, norms,
    v, dr, reg, msk, con, ws, wa,
    halo_p, halo_n, reg_p, reg_n, col_l, col_r, reg_l, reg_r,
    x, s, y, nl, flux, par, ar_x, ar_y, mine,
    sem_v, sem_d, sem_s, send_h, recv_h, send_c, recv_c, send_y, recv_y, send_x, recv_x,
):
    gx, gy = lax.axis_index("gx"), lax.axis_index("gy")
    up, down = lax.rem(gx + 1, nx), lax.rem(gx + nx - 1, nx)
    right, left = lax.rem(gy + 1, ny), lax.rem(gy + ny - 1, ny)

    barrier = pltpu.get_barrier_semaphore()

    def greet_x(i, c):
        pl.semaphore_signal(barrier, inc=1, device_id={"gx": lax.rem(gx + i, nx)}, device_id_type=MESH)
        return c

    def greet_y(i, c):
        pl.semaphore_signal(barrier, inc=1, device_id={"gy": lax.rem(gy + i, ny)}, device_id_type=MESH)
        return c

    lax.fori_loop(1, nx, greet_x, 0)
    lax.fori_loop(1, ny, greet_y, 0)

    small = [
        pltpu.make_async_copy(region, reg, sem_s.at[0]),
        pltpu.make_async_copy(mask, msk, sem_s.at[1]),
        pltpu.make_async_copy(ws_hbm, ws, sem_s.at[2]),
        pltpu.make_async_copy(wa_hbm, wa, sem_s.at[3]),
    ]
    for copy in small:
        copy.start()

    def load_row(r, c):
        for zt in range(ZT):
            pltpu.make_async_copy(
                volt.at[r, :, pl.ds(zt * LANES, LANES)],
                v.at[r, zt, pl.ds(PAD, cols), :],
                sem_v.at[r],
            ).start()
        pltpu.make_async_copy(drive.at[r], dr.at[r], sem_d.at[r]).start()
        return c

    lax.fori_loop(0, rows, load_row, 0)

    pl.semaphore_wait(barrier, nx + ny - 2)
    sends = []

    def send(src, dst, ssem, rsem, where):
        copy = pltpu.make_async_remote_copy(
            src_ref=src, dst_ref=dst, send_sem=ssem, recv_sem=rsem,
            device_id=where, device_id_type=MESH,
        )
        copy.start()
        sends.append(copy)
        return copy

    to_right = [
        send(volt.at[:, pl.ds(cols - 1, 1), :], col_l, send_c.at[0], recv_c.at[0], {"gy": right}),
        send(region.at[:, pl.ds(cols - 8, 8), :], reg_l, send_c.at[1], recv_c.at[1], {"gy": right}),
    ]
    to_left = [
        send(volt.at[:, pl.ds(0, 1), :], col_r, send_c.at[2], recv_c.at[2], {"gy": left}),
        send(region.at[:, pl.ds(0, 8), :], reg_r, send_c.at[3], recv_c.at[3], {"gy": left}),
    ]
    reg_up = send(region.at[rows - 1], reg_p, send_h.at[0, CHUNKS], recv_h.at[0, CHUNKS], {"gx": up})
    reg_down = send(region.at[0], reg_n, send_h.at[1, CHUNKS], recv_h.at[1, CHUNKS], {"gx": down})
    piece = cols // CHUNKS
    ups, downs = [], []
    for k in range(CHUNKS):
        part = pl.ds(k * piece, piece)
        ups.append(send(volt.at[rows - 1, part, :], halo_p.at[part, :], send_h.at[0, k], recv_h.at[0, k], {"gx": up}))
        downs.append(send(volt.at[0, part, :], halo_n.at[part, :], send_h.at[1, k], recv_h.at[1, k], {"gx": down}))

    lane = lax.broadcasted_iota(jnp.int32, (8, LANES), 1)
    high = (lane >= KC).astype(jnp.int32)
    coef = lane % KC
    order = (coef % H + 1).astype(F32) * BASE_FREQ
    freq = jnp.where(coef < H, order, -order)
    partner = jnp.where(coef < H, lane + H, lane - H)
    own = [high + 2 * zt for zt in range(ZT)]
    within = [jnp.full((8, LANES), 2 * zt, jnp.int32) for zt in range(ZT)]
    across = [jnp.where(high == 0, 2 * zt - 1 if zt else NZ - 1, 2 * zt + 1) for zt in range(ZT)]
    left_half = lax.broadcasted_iota(jnp.int32, (cols, LANES), 1) < KC

    edge = jnp.zeros((PAD, LANES), F32)

    def clear(r, c):
        for zt in range(ZT):
            v[r, zt, pl.ds(0, PAD), :] = edge
            v[r, zt, pl.ds(cols + PAD, PAD), :] = edge
        return c

    lax.fori_loop(0, rows, clear, 0)
    flux[...] = jnp.zeros_like(flux)

    small[0].wait()

    def conduct_row(r, c):
        con[r] = pick(reg[r], sigma)
        return c

    lax.fori_loop(0, rows, conduct_row, 0)
    for copy in small[1:]:
        copy.wait()

    def wait_volt(r):
        whole = v.at[r, :, pl.ds(PAD, cols), :]
        pltpu.make_async_copy(whole, whole, sem_v.at[r]).wait()

    wait_volt(0)

    def one_row(r, c):
        after = jnp.minimum(r + 1, rows - 1)

        @pl.when(r < rows - 1)
        def _():
            wait_volt(r + 1)

        pltpu.make_async_copy(dr.at[r], dr.at[r], sem_d.at[r]).wait()

        here = widen(con[r])
        there = widen(con[after])
        live = jnp.where(r < rows - 1, 1.0, 0.0)
        col = lax.broadcasted_iota(jnp.int32, (cols, LANES), 0)
        z_lane = lax.broadcasted_iota(jnp.int32, (cols, LANES), 1)
        cell = z_lane < NZ
        par[0] = jnp.where(cell, harmonic_mean(here, there), 0.0) * live
        nxt = jnp.where(col == cols - 1, 0.0, pltpu.roll(here, cols - 1, 0))
        col_next = jnp.where(cell, harmonic_mean(here, nxt), 0.0)
        par[1] = col_next
        par[2] = jnp.where(col == 0, 0.0, pltpu.roll(col_next, 1, 0))
        deep = pltpu.roll(here, LANES - 1, 1)
        par[3] = jnp.where(z_lane < NZ - 1, harmonic_mean(here, deep), 0.0)
        par[4] = widen(pick(reg[r], cap))
        par[5] = widen(msk[r].astype(F32) * 0.5)

        for zt in range(ZT):
            value = v[r, zt, pl.ds(PAD, cols), :]
            near = value.astype(BF16).astype(F32)
            rest = value - near
            x[pl.ds(zt * cols, cols), :] = jnp.where(left_half, near, pltpu.roll(rest, KC, 1)).astype(BF16)
            x[pl.ds((ZT + zt) * cols, cols), :] = jnp.where(left_half, pltpu.roll(near, KC, 1), rest).astype(BF16)
        xs = x[...]
        s[...] = jnp.dot(jnp.concatenate([xs, xs], axis=1), ws[...], preferred_element_type=F32)
        for zt in range(ZT):
            for half in range(2):
                wave = s[pl.ds((half * ZT + zt) * cols, cols), :]
                bent = jnp.tanh(wave)
                soft = jnp.abs(wave) - jnp.log(1.0 + jnp.abs(bent))
                y[pl.ds(zt * cols, cols), pl.ds(half * 2 * S, S)] = soft.astype(BF16)
                y[pl.ds(zt * cols, cols), pl.ds(half * 2 * S + S, S)] = bent.astype(BF16)
        full = jnp.dot(y[...], wa[...], preferred_element_type=F32)
        nl[...] = full[:, :LANES] + full[:, LANES:]

        for j in range(cols // 8):
            g_row, g_next, g_prev, g_deep, capacity, diode = (par[i, pl.ds(8 * j, 8), :] for i in range(6))
            values = [v[r, zt, pl.ds(PAD + 8 * j, 8), :] for zt in range(ZT)]
            turned = [pltpu.roll(value, KC, 1) for value in values]
            for zt in range(ZT):
                value = values[zt]
                lanes = pl.ds(zt * LANES, LANES)
                spot = pl.ds(8 * j, 8)
                flow = spread(g_row, own[zt]) * (value - v[after, zt, pl.ds(PAD + 8 * j, 8), :])
                total = flow - flux[spot, lanes] - dr[r, spot, lanes]
                flux[spot, lanes] = flow
                total += spread(g_next, own[zt]) * (value - v[r, zt, pl.ds(PAD + 8 * j + 1, 8), :])
                total += spread(g_prev, own[zt]) * (value - v[r, zt, pl.ds(PAD + 8 * j - 1, 8), :])
                total += spread(g_deep, within[zt]) * (value - turned[zt])
                outer = jnp.where(high == 0, turned[max(zt - 1, 0)], turned[min(zt + 1, ZT - 1)])
                total += spread(g_deep, across[zt]) * (value - outer)
                total += spread(capacity, own[zt]) * (freq * spread(value, partner))
                total += spread(diode, own[zt]) * (value + nl[pl.ds(zt * cols + 8 * j, 8), :])
                out[r, spot, lanes] = total
        return c

    lax.fori_loop(0, rows, one_row, 0)

    for copy in to_right + to_left:
        copy.wait_recv()
    sub = lax.broadcasted_iota(jnp.int32, (8, LANES), 0)

    def fix_cols(r, acc):
        first = widen(con[r, pl.ds(0, 8), :])
        last = widen(con[r, pl.ds(cols - 8, 8), :])
        before = widen(pltpu.roll(pick(reg_l[r], sigma), 1, 0))
        behind = widen(pltpu.roll(pick(reg_r[r], sigma), 7, 0))
        g_l = jnp.where((sub == 0) & (lane < NZ) & (gy > 0), harmonic_mean(first, before), 0.0)
        g_r = jnp.where((sub == 7) & (lane < NZ) & (gy < ny - 1), harmonic_mean(last, behind), 0.0)
        for zt in range(ZT):
            lanes = pl.ds(zt * LANES, LANES)
            out[r, pl.ds(0, 8), lanes] += spread(g_l, own[zt]) * (
                v[r, zt, pl.ds(PAD, 8), :] - jnp.broadcast_to(col_l[r, :, lanes], (8, LANES))
            )
            out[r, pl.ds(cols - 8, 8), lanes] += spread(g_r, own[zt]) * (
                v[r, zt, pl.ds(PAD + cols - 8, 8), :] - jnp.broadcast_to(col_r[r, :, lanes], (8, LANES))
            )
        return acc

    lax.fori_loop(0, rows, fix_cols, 0)

    def squares(r, acc):
        parts = [jnp.zeros((8, LANES), F32) for _ in range(4)]
        for zt in range(ZT):
            for j in range(cols // 8):
                value = out[r, pl.ds(8 * j, 8), pl.ds(zt * LANES, LANES)]
                parts[j % 4] = parts[j % 4] + value * value
        return acc + ((parts[0] + parts[1]) + (parts[2] + parts[3]))

    acc = lax.fori_loop(1, rows - 1, squares, jnp.zeros((8, LANES), F32))

    for copies, notice, r, halo, marks in ((ups, reg_up, 0, halo_p, reg_p), (downs, reg_down, rows - 1, halo_n, reg_n)):
        notice.wait_recv()
        par[r // (rows - 1)] = jnp.where(
            lax.broadcasted_iota(jnp.int32, (cols, LANES), 1) < NZ,
            harmonic_mean(widen(con[r]), widen(pick(marks[...], sigma))),
            0.0,
        )
    for k in range(CHUNKS):
        for copies, r, halo in ((ups, 0, halo_p), (downs, rows - 1, halo_n)):
            copies[k].wait_recv()

            def fix_row(j, acc, r=r, halo=halo):
                base = pl.multiple_of(8 * j, 8)
                spot = pl.ds(base, 8)
                gain = par[r // (rows - 1), spot, :]
                parts = [jnp.zeros((8, LANES), F32) for _ in range(4)]
                for zt in range(ZT):
                    lanes = pl.ds(zt * LANES, LANES)
                    value = out[r, spot, lanes] + spread(gain, own[zt]) * (
                        v[r, zt, pl.ds(base + PAD, 8), :] - halo[spot, lanes]
                    )
                    out[r, spot, lanes] = value
                    parts[zt % 4] = parts[zt % 4] + value * value
                return acc + ((parts[0] + parts[1]) + (parts[2] + parts[3]))

            acc = lax.fori_loop(k * piece // 8, (k + 1) * piece // 8, fix_row, acc)

    local = jnp.sum(acc, axis=0, keepdims=True)
    mine[0] = local + pltpu.roll(local, KC, 1)

    def reduce_over(name, here, count, buf, slot, ssems, rsems):
        buf[here] = mine[slot]

        def copy_of(i):
            return pltpu.make_async_remote_copy(
                src_ref=mine.at[slot], dst_ref=buf.at[here], send_sem=ssems.at[i], recv_sem=rsems.at[i],
                device_id={name: lax.rem(here + i, count)}, device_id_type=MESH,
            )

        def begin(i, c):
            copy_of(i).start()
            return c

        def finish(i, c):
            copy_of(i).wait()
            return c

        lax.fori_loop(1, count, begin, 0)
        lax.fori_loop(1, count, finish, 0)
        total = buf[0]
        for i in range(1, count):
            total = total + buf[i]
        return total

    mine[1] = reduce_over("gy", gy, ny, ar_y, 0, send_y, recv_y)
    total = reduce_over("gx", gx, nx, ar_x, 1, send_x, recv_x)
    norms[...] = jnp.sqrt(total / cells + NORM_EPS)

    for copy in sends:
        copy.wait_send()


def body(nx, ny, volt, drive, region, diode_mask, sigma_table, cap_table):
    rows, cols, width = volt.shape
    cells = rows * cols * NZ * nx * ny
    ws, wa = spectral_tables()
    anywhere = pl.BlockSpec(memory_space=pl.ANY)
    smem = pl.BlockSpec(memory_space=pltpu.SMEM)
    vmem = pl.BlockSpec(memory_space=pltpu.VMEM)
    dma = pltpu.SemaphoreType.DMA
    residual, norms = pl.pallas_call(
        functools.partial(kernel, nx, ny, rows, cols, cells),
        out_shape=(
            jax.ShapeDtypeStruct((rows, cols, width), F32),
            jax.ShapeDtypeStruct((1, LANES), F32),
        ),
        in_specs=[anywhere] * 4 + [smem] * 2 + [anywhere] * 2,
        out_specs=(vmem, vmem),
        scratch_shapes=[
            pltpu.VMEM((rows, ZT, cols + 2 * PAD, LANES), F32),
            pltpu.VMEM((rows, cols, width), F32),
            pltpu.VMEM((rows, cols, NZ), jnp.int32),
            pltpu.VMEM((rows, cols, NZ), jnp.int32),
            pltpu.VMEM((rows, cols, NZ), F32),
            pltpu.VMEM(ws.shape, BF16),
            pltpu.VMEM(wa.shape, BF16),
            pltpu.VMEM((cols, width), F32),
            pltpu.VMEM((cols, width), F32),
            pltpu.VMEM((cols, NZ), jnp.int32),
            pltpu.VMEM((cols, NZ), jnp.int32),
            pltpu.VMEM((rows, 1, width), F32),
            pltpu.VMEM((rows, 1, width), F32),
            pltpu.VMEM((rows, 8, NZ), jnp.int32),
            pltpu.VMEM((rows, 8, NZ), jnp.int32),
            pltpu.VMEM((2 * ZT * cols, LANES), BF16),
            pltpu.VMEM((2 * ZT * cols, S), F32),
            pltpu.VMEM((ZT * cols, 4 * S), BF16),
            pltpu.VMEM((ZT * cols, LANES), F32),
            pltpu.VMEM((cols, width), F32),
            pltpu.VMEM((6, cols, LANES), F32),
            pltpu.VMEM((nx, 1, LANES), F32),
            pltpu.VMEM((ny, 1, LANES), F32),
            pltpu.VMEM((2, 1, LANES), F32),
            dma((rows,)), dma((rows,)), dma((4,)),
            dma((2, CHUNKS + 1)), dma((2, CHUNKS + 1)),
            dma((4,)), dma((4,)),
            dma((ny,)), dma((ny,)), dma((nx,)), dma((nx,)),
        ],
        compiler_params=pltpu.CompilerParams(
            collective_id=0, has_side_effects=True, vmem_limit_bytes=60 * 1024 * 1024
        ),
        name="residual",
    )(volt, drive, region, diode_mask, sigma_table, cap_table, ws, wa)
    return residual, norms[0, :KC]


def solution(mesh):
    nx, ny = mesh.shape["gx"], mesh.shape["gy"]
    cut = P("gx", "gy", None)
    return jax.shard_map(
        functools.partial(body, nx, ny), mesh=mesh, in_specs=(cut, cut, cut, cut, P(), P()),
        out_specs=(cut, P()), check_vma=False,
    )
```

```python
import functools
import math

import jax
import jax.numpy as jnp
import numpy as np
from jax import lax
from jax.experimental import pallas as pl
from jax.experimental.pallas import tpu as pltpu
from jax.sharding import PartitionSpec as P

NZ = 32
H = 32
KC = 64
S = 256
REGIONS = 8
BASE_FREQ = 0.1
NORM_EPS = 1e-06
LANES = 128
ZT = NZ * KC // LANES
PAD = 8
CHUNKS = 4
SEND_AT = 1

MESH = pl.DeviceIdType.MESH
F32 = jnp.float32
BF16 = jnp.bfloat16


def split(table):
    high = table.astype(jnp.bfloat16)
    low = (table - high.astype(np.float64)).astype(jnp.bfloat16)
    return high, low


def spectral_tables():
    orders = np.arange(1, H + 1, dtype=np.float64)
    steps = np.arange(S, dtype=np.int64)
    angles = 2.0 * math.pi * ((orders[:, None].astype(np.int64) * steps[None, :]) % S) / S
    cosines, sines = np.cos(angles), np.sin(angles)
    synthesis = np.concatenate([cosines, sines], axis=0)
    analysis = synthesis.T * (2.0 / S)
    freq = BASE_FREQ * orders
    derived = np.concatenate([freq * analysis[:, H:], -freq * analysis[:, :H]], axis=1)
    high, low = split(synthesis)
    ws = np.concatenate([high, high, low, low], axis=0)
    both = np.concatenate([analysis, derived], axis=0)
    high, low = split(both)
    wa = np.zeros((2, 2 * S, 2, LANES), jnp.bfloat16)
    for half in range(2):
        wa[half, :, 0, half * KC : half * KC + KC] = high
        wa[half, :, 1, half * KC : half * KC + KC] = low
    return ws, wa.reshape(4 * S, 2 * LANES)


def harmonic_mean(left, right):
    return 2.0 * left * right / (left + right)


def pick(region, table):
    value = jnp.full(region.shape, table[0], F32)
    for idx in range(1, REGIONS):
        value = jnp.where(region == idx, table[idx], value)
    return value


def widen(compact):
    rows, count = compact.shape
    return jnp.concatenate([compact, jnp.zeros((rows, LANES - count), compact.dtype)], axis=1)


def spread(compact, index):
    return jnp.take_along_axis(compact, index, axis=1, mode="promise_in_bounds")


def kernel(
    nx, ny, rows, cols, cells,
    volt, drive, region, mask, sigma, cap, ws_hbm, wa_hbm,
    out, norms,
    v, dr, reg, msk, ws, wa,
    halo_p, halo_n, reg_p, reg_n, col_l, col_r, con_l, con_r,
    x, s, y, nl, flux, turned, swapped, par, gain, ar_x, ar_y, mine,
    sem_v, sem_d, sem_s, send_h, recv_h, send_c, recv_c, send_y, recv_y, send_x, recv_x,
):
    gx, gy = lax.axis_index("gx"), lax.axis_index("gy")
    up, down = lax.rem(gx + 1, nx), lax.rem(gx + nx - 1, nx)
    right, left = lax.rem(gy + 1, ny), lax.rem(gy + ny - 1, ny)
    groups = cols // 8

    barrier = pltpu.get_barrier_semaphore()
    for i in range(1, nx):
        pl.semaphore_signal(barrier, inc=1, device_id={"gx": lax.rem(gx + i, nx)}, device_id_type=MESH)
    for i in range(1, ny):
        pl.semaphore_signal(barrier, inc=1, device_id={"gy": lax.rem(gy + i, ny)}, device_id_type=MESH)

    small = [
        pltpu.make_async_copy(region, reg, sem_s.at[0]),
        pltpu.make_async_copy(mask, msk, sem_s.at[1]),
        pltpu.make_async_copy(ws_hbm, ws, sem_s.at[2]),
        pltpu.make_async_copy(wa_hbm, wa, sem_s.at[3]),
    ]
    for copy in small:
        copy.start()

    def load_row(r, c):
        for zt in range(ZT):
            pltpu.make_async_copy(
                volt.at[r, :, pl.ds(zt * LANES, LANES)],
                v.at[r, zt, pl.ds(PAD, cols), :],
                sem_v.at[r],
            ).start()
        pltpu.make_async_copy(drive.at[r], dr.at[r], sem_d.at[r]).start()
        return c

    lax.fori_loop(0, rows, load_row, 0)

    def wait_volt(r):
        whole = v.at[r, :, pl.ds(PAD, cols), :]
        pltpu.make_async_copy(whole, whole, sem_v.at[r]).wait()

    def remote(src, dst, ssem, rsem, where):
        return pltpu.make_async_remote_copy(
            src_ref=src, dst_ref=dst, send_sem=ssem, recv_sem=rsem,
            device_id=where, device_id_type=MESH,
        )

    piece = cols // CHUNKS
    col_copies = [
        remote(volt.at[:, pl.ds(cols - 1, 1), :], col_l, send_c.at[0], recv_c.at[0], {"gy": right}),
        remote(par.at[:, 6, pl.ds(cols - 1, 1), :], con_l, send_c.at[1], recv_c.at[1], {"gy": right}),
        remote(volt.at[:, pl.ds(0, 1), :], col_r, send_c.at[2], recv_c.at[2], {"gy": left}),
        remote(par.at[:, 6, pl.ds(0, 1), :], con_r, send_c.at[3], recv_c.at[3], {"gy": left}),
    ]
    reg_copies = [
        remote(region.at[rows - 1], reg_p, send_h.at[0, CHUNKS], recv_h.at[0, CHUNKS], {"gx": up}),
        remote(region.at[0], reg_n, send_h.at[1, CHUNKS], recv_h.at[1, CHUNKS], {"gx": down}),
    ]
    row_copies = []
    for k in range(CHUNKS):
        part = pl.ds(k * piece, piece)
        row_copies.append((
            remote(volt.at[rows - 1, part, :], halo_p.at[part, :], send_h.at[0, k], recv_h.at[0, k], {"gx": up}),
            remote(volt.at[0, part, :], halo_n.at[part, :], send_h.at[1, k], recv_h.at[1, k], {"gx": down}),
        ))
    sends = reg_copies + col_copies + [copy for pair in row_copies for copy in pair]

    lane = lax.broadcasted_iota(jnp.int32, (8, LANES), 1)
    high = (lane >= KC).astype(jnp.int32)
    coef = lane % KC
    order = (coef % H + 1).astype(F32) * BASE_FREQ
    freq = jnp.where(coef < H, order, -order)
    partner = jnp.where(coef < H, lane + H, lane - H)
    own = [high + 2 * zt for zt in range(ZT)]
    within = [jnp.full((8, LANES), 2 * zt, jnp.int32) for zt in range(ZT)]
    across = [jnp.where(high == 0, 2 * zt - 1 if zt else NZ - 1, 2 * zt + 1) for zt in range(ZT)]
    left_half = lax.broadcasted_iota(jnp.int32, (cols, LANES), 1) < KC

    edge = jnp.zeros((PAD, LANES), F32)

    def clear(r, c):
        for zt in range(ZT):
            v[r, zt, pl.ds(0, PAD), :] = edge
            v[r, zt, pl.ds(cols + PAD, PAD), :] = edge
        return c

    lax.fori_loop(0, rows, clear, 0)
    flux[...] = jnp.zeros_like(flux)

    small[0].wait()
    small[1].wait()

    pairs = rows // 2
    pair_lane = lax.broadcasted_iota(jnp.int32, (NZ, LANES), 1)
    layer = lax.broadcasted_iota(jnp.int32, (NZ, LANES), 0)
    pair_regions = [jnp.concatenate([reg[2 * p], reg[2 * p + 1]], axis=1) for p in range(pairs)]
    conduct = [pick(both, sigma) for both in pair_regions]
    for p in range(pairs):
        here = conduct[p]
        beyond = pltpu.roll(conduct[p + 1], cols, 1) if p + 1 < pairs else jnp.zeros_like(here)
        there = jnp.where(pair_lane < cols, pltpu.roll(here, cols, 1), beyond)
        after = jnp.where(pair_lane % cols == cols - 1, 0.0, pltpu.roll(here, LANES - 1, 1))
        deeper = jnp.where(layer == NZ - 1, 0.0, pltpu.roll(here, NZ - 1, 0))
        g_next = harmonic_mean(here, after)
        diode = jnp.concatenate([msk[2 * p], msk[2 * p + 1]], axis=1).astype(F32) * 0.5
        fields = (
            harmonic_mean(here, there), g_next, pltpu.roll(g_next, 1, 1), harmonic_mean(here, deeper),
            pick(pair_regions[p], cap), diode, here,
        )
        for i, field in enumerate(fields):
            flat = widen(jnp.transpose(field))
            par[2 * p, i] = flat[:cols]
            par[2 * p + 1, i] = flat[cols:]
    for copy in small[2:]:
        copy.wait()
    wait_volt(0)

    def one_row(r, c):
        after = jnp.minimum(r + 1, rows - 1)

        @pl.when(r == SEND_AT)
        def _():
            pl.semaphore_wait(barrier, nx + ny - 2)
            for copy in sends:
                copy.start()

        @pl.when(r < rows - 1)
        def _():
            wait_volt(r + 1)

        pltpu.make_async_copy(dr.at[r], dr.at[r], sem_d.at[r]).wait()

        for zt in range(ZT):
            value = v[r, zt, pl.ds(PAD, cols), :]
            near = value.astype(BF16).astype(F32)
            rest = value - near
            x[pl.ds(zt * cols, cols), :] = jnp.where(left_half, near, pltpu.roll(rest, KC, 1)).astype(BF16)
            x[pl.ds((ZT + zt) * cols, cols), :] = jnp.where(left_half, pltpu.roll(near, KC, 1), rest).astype(BF16)
            turned[zt] = pltpu.roll(value, KC, 1)
            for j in range(groups):
                swapped[zt, pl.ds(8 * j, 8), :] = freq * spread(value[8 * j : 8 * j + 8], partner)
        xs = x[...]
        s[...] = jnp.dot(jnp.concatenate([xs, xs], axis=1), ws[...], preferred_element_type=F32)
        for zt in range(ZT):
            for half in range(2):
                wave = s[pl.ds((half * ZT + zt) * cols, cols), :]
                bent = jnp.tanh(wave)
                soft = jnp.abs(wave) - jnp.log(1.0 + jnp.abs(bent))
                y[pl.ds(zt * cols, cols), pl.ds(half * 2 * S, S)] = soft.astype(BF16)
                y[pl.ds(zt * cols, cols), pl.ds(half * 2 * S + S, S)] = bent.astype(BF16)
        full = jnp.dot(y[...], wa[...], preferred_element_type=F32)
        nl[...] = full[:, :LANES] + full[:, LANES:]

        for zt in range(ZT):
            lanes = pl.ds(zt * LANES, LANES)

            def gains(i, index):
                return [spread(par[r, i, pl.ds(8 * j, 8), :], index) for j in range(groups)]

            g_row, g_next, g_prev = gains(0, own[zt]), gains(1, own[zt]), gains(2, own[zt])
            capacity, diode = gains(4, own[zt]), gains(5, own[zt])
            g_in, g_out = gains(3, within[zt]), gains(3, across[zt])
            for j in range(groups):
                spot = pl.ds(8 * j, 8)
                value = v[r, zt, pl.ds(PAD + 8 * j, 8), :]
                flow = g_row[j] * (value - v[after, zt, pl.ds(PAD + 8 * j, 8), :])
                total = flow - flux[spot, lanes] - dr[r, spot, lanes]
                flux[spot, lanes] = flow
                total += g_next[j] * (value - v[r, zt, pl.ds(PAD + 8 * j + 1, 8), :])
                total += g_prev[j] * (value - v[r, zt, pl.ds(PAD + 8 * j - 1, 8), :])
                total += g_in[j] * (value - turned[zt, spot, :])
                outer = jnp.where(high == 0, turned[max(zt - 1, 0), spot, :], turned[min(zt + 1, ZT - 1), spot, :])
                total += g_out[j] * (value - outer)
                total += capacity[j] * swapped[zt, spot, :]
                total += diode[j] * (value + nl[pl.ds(zt * cols + 8 * j, 8), :])
                out[r, spot, lanes] = total
        return c

    lax.fori_loop(0, rows, one_row, 0)

    for copy in col_copies:
        copy.wait_recv()
    sub = lax.broadcasted_iota(jnp.int32, (8, LANES), 0)

    def fix_cols(r, c):
        first = par[r, 6, pl.ds(0, 8), :]
        last = par[r, 6, pl.ds(cols - 8, 8), :]
        before = jnp.broadcast_to(con_l[r], (8, LANES))
        behind = jnp.broadcast_to(con_r[r], (8, LANES))
        g_l = jnp.where((sub == 0) & (lane < NZ) & (gy > 0), harmonic_mean(first, before), 0.0)
        g_r = jnp.where((sub == 7) & (lane < NZ) & (gy < ny - 1), harmonic_mean(last, behind), 0.0)
        for zt in range(ZT):
            lanes = pl.ds(zt * LANES, LANES)
            out[r, pl.ds(0, 8), lanes] += spread(g_l, own[zt]) * (
                v[r, zt, pl.ds(PAD, 8), :] - jnp.broadcast_to(col_l[r, :, lanes], (8, LANES))
            )
            out[r, pl.ds(cols - 8, 8), lanes] += spread(g_r, own[zt]) * (
                v[r, zt, pl.ds(PAD + cols - 8, 8), :] - jnp.broadcast_to(col_r[r, :, lanes], (8, LANES))
            )
        return c

    lax.fori_loop(0, rows, fix_cols, 0)

    def squares(r, acc):
        parts = [jnp.zeros((8, LANES), F32) for _ in range(8)]
        for zt in range(ZT):
            for j in range(groups):
                value = out[r, pl.ds(8 * j, 8), pl.ds(zt * LANES, LANES)]
                parts[j % 8] = parts[j % 8] + value * value
        while len(parts) > 1:
            parts = [a + b for a, b in zip(parts[::2], parts[1::2])]
        return acc + parts[0]

    acc = lax.fori_loop(1, rows - 1, squares, jnp.zeros((8, LANES), F32))

    for end, (copy, marks, r) in enumerate(zip(reg_copies, (reg_p, reg_n), (0, rows - 1))):
        copy.wait_recv()
        field = jnp.concatenate([pick(marks[...], sigma), jnp.zeros((NZ, LANES - cols), F32)], axis=1)
        flat = widen(jnp.transpose(field))[:cols]
        inside = lax.broadcasted_iota(jnp.int32, (cols, LANES), 1) < NZ
        gain[end] = jnp.where(inside, harmonic_mean(par[r, 6], flat), 0.0)
    for k in range(CHUNKS):
        for end, (copy, halo, r) in enumerate(zip(row_copies[k], (halo_p, halo_n), (0, rows - 1))):
            copy.wait_recv()
            parts = [jnp.zeros((8, LANES), F32) for _ in range(8)]
            for j in range(k * piece // 8, (k + 1) * piece // 8):
                spot = pl.ds(8 * j, 8)
                for zt in range(ZT):
                    lanes = pl.ds(zt * LANES, LANES)
                    value = out[r, spot, lanes] + spread(gain[end, spot, :], own[zt]) * (
                        v[r, zt, pl.ds(8 * j + PAD, 8), :] - halo[spot, lanes]
                    )
                    out[r, spot, lanes] = value
                    parts[zt % 8] = parts[zt % 8] + value * value
            while len(parts) > 1:
                parts = [a + b for a, b in zip(parts[::2], parts[1::2])]
            acc = acc + parts[0]

    local = jnp.sum(acc, axis=0, keepdims=True)

    def reduce_over(name, here, count, value, buf, slot, ssem, rsem):
        mine[slot] = value
        buf[pl.ds(here, 1), :] = value
        for i in range(1, count):
            remote(mine.at[slot], buf.at[pl.ds(here, 1), :], ssem, rsem, {name: lax.rem(here + i, count)}).start()
        others = buf.at[pl.ds(0, count - 1), :]
        pltpu.make_async_copy(others, others, rsem).wait()
        return jnp.sum(buf[...], axis=0, keepdims=True)

    value = reduce_over("gy", gy, ny, local + pltpu.roll(local, KC, 1), ar_y, 0, send_y, recv_y)
    value = reduce_over("gx", gx, nx, value, ar_x, 1, send_x, recv_x)
    norms[...] = jnp.sqrt(value / cells + NORM_EPS)[0, :KC]

    for count, buf, ssem in ((ny, ar_y, send_y), (nx, ar_x, send_x)):
        others = buf.at[pl.ds(0, count - 1), :]
        pltpu.make_async_copy(others, others, ssem).wait()
    for copy in sends:
        copy.wait_send()


def body(nx, ny, volt, drive, region, diode_mask, sigma_table, cap_table):
    rows, cols, width = volt.shape
    cells = rows * cols * NZ * nx * ny
    ws, wa = spectral_tables()
    hbm = pl.BlockSpec(memory_space=pltpu.HBM)
    smem = pl.BlockSpec(memory_space=pltpu.SMEM)
    vmem = pl.BlockSpec(memory_space=pltpu.VMEM)
    dma = pltpu.SemaphoreType.DMA
    held = functools.partial(pltpu.with_memory_space_constraint, memory_space=pltpu.HBM)
    return pl.pallas_call(
        functools.partial(kernel, nx, ny, rows, cols, cells),
        out_shape=(
            jax.ShapeDtypeStruct((rows, cols, width), F32),
            jax.ShapeDtypeStruct((KC,), F32),
        ),
        in_specs=[hbm] * 4 + [smem] * 2 + [hbm] * 2,
        out_specs=(vmem, vmem),
        scratch_shapes=[
            pltpu.VMEM((rows, ZT, cols + 2 * PAD, LANES), F32),
            pltpu.VMEM((rows, cols, width), F32),
            pltpu.VMEM((rows, NZ, cols), jnp.int32),
            pltpu.VMEM((rows, NZ, cols), jnp.int32),
            pltpu.VMEM(ws.shape, BF16),
            pltpu.VMEM(wa.shape, BF16),
            pltpu.VMEM((cols, width), F32),
            pltpu.VMEM((cols, width), F32),
            pltpu.VMEM((NZ, cols), jnp.int32),
            pltpu.VMEM((NZ, cols), jnp.int32),
            pltpu.VMEM((rows, 1, width), F32),
            pltpu.VMEM((rows, 1, width), F32),
            pltpu.VMEM((rows, 1, LANES), F32),
            pltpu.VMEM((rows, 1, LANES), F32),
            pltpu.VMEM((2 * ZT * cols, LANES), BF16),
            pltpu.VMEM((2 * ZT * cols, S), F32),
            pltpu.VMEM((ZT * cols, 4 * S), BF16),
            pltpu.VMEM((ZT * cols, LANES), F32),
            pltpu.VMEM((cols, width), F32),
            pltpu.VMEM((ZT, cols, LANES), F32),
            pltpu.VMEM((ZT, cols, LANES), F32),
            pltpu.VMEM((rows, 7, cols, LANES), F32),
            pltpu.VMEM((2, cols, LANES), F32),
            pltpu.VMEM((nx, LANES), F32),
            pltpu.VMEM((ny, LANES), F32),
            pltpu.VMEM((2, 1, LANES), F32),
            dma((rows,)), dma((rows,)), dma((4,)),
            dma((2, CHUNKS + 1)), dma((2, CHUNKS + 1)),
            dma((4,)), dma((4,)),
            dma, dma, dma, dma,
        ],
        compiler_params=pltpu.CompilerParams(
            collective_id=0, has_side_effects=True, vmem_limit_bytes=38 * 1024 * 1024
        ),
        name="residual",
    )(
        held(volt), held(drive), held(jnp.swapaxes(region, 1, 2)), held(jnp.swapaxes(diode_mask, 1, 2)),
        sigma_table, cap_table, held(ws), held(wa),
    )


def solution(mesh):
    nx, ny = mesh.shape["gx"], mesh.shape["gy"]
    cut = P("gx", "gy", None)
    return jax.shard_map(
        functools.partial(body, nx, ny), mesh=mesh, in_specs=(cut, cut, cut, cut, P(), P()),
        out_specs=(cut, P()), check_vma=False,
    )
```

```python
import functools
import math

import jax
import jax.numpy as jnp
import numpy as np
from jax import lax
from jax.experimental import pallas as pl
from jax.experimental.pallas import tpu as pltpu
from jax.sharding import PartitionSpec as P

NZ = 32
H = 32
KC = 64
S = 256
REGIONS = 8
BASE_FREQ = 0.1
NORM_EPS = 1e-06
LANES = 128
ZT = NZ * KC // LANES
INNER = 4
PAD = 8
CHUNKS = 4
SEND_AT = 1

MESH = pl.DeviceIdType.MESH
F32 = jnp.float32
BF16 = jnp.bfloat16


def split(table):
    high = table.astype(jnp.bfloat16)
    low = (table - high.astype(np.float64)).astype(jnp.bfloat16)
    return high, low


def spectral_tables():
    orders = np.arange(1, H + 1, dtype=np.float64)
    steps = np.arange(S, dtype=np.int64)
    angles = 2.0 * math.pi * ((orders[:, None].astype(np.int64) * steps[None, :]) % S) / S
    cosines, sines = np.cos(angles), np.sin(angles)
    synthesis = np.concatenate([cosines, sines], axis=0)
    analysis = synthesis.T * (2.0 / S)
    freq = BASE_FREQ * orders
    derived = np.concatenate([freq * analysis[:, H:], -freq * analysis[:, :H]], axis=1)
    high, low = split(synthesis)
    ws = np.concatenate([high, high, low, low], axis=0)
    both = 0.5 * np.concatenate([analysis, derived], axis=0)
    high, low = split(both)
    wa = np.zeros((2, 2 * S, 2, LANES), jnp.bfloat16)
    for half in range(2):
        wa[half, :, 0, half * KC : half * KC + KC] = high
        wa[half, :, 1, half * KC : half * KC + KC] = low
    return ws, wa.reshape(4 * S, 2 * LANES)


def harmonic_mean(left, right):
    return 2.0 * left * right / (left + right)


def pick(region, table):
    value = jnp.full(region.shape, table[0], F32)
    for idx in range(1, REGIONS):
        value = jnp.where(region == idx, table[idx], value)
    return value


def widen(compact):
    rows, count = compact.shape
    return jnp.concatenate([compact, jnp.zeros((rows, LANES - count), compact.dtype)], axis=1)


def spread(compact, index):
    return jnp.take_along_axis(compact, index, axis=1, mode="promise_in_bounds")


def kernel(
    nx, ny, rows, cols, cells,
    volt, drive, region, mask, sigma_hbm, cap_hbm, ws_hbm, wa_hbm,
    out, norms,
    sigma, cap, v, dr, reg, msk, ws, wa,
    halo_p, halo_n, reg_p, reg_n, col_l, col_r, con_l, con_r,
    x, s, y, nl, flux, side, turned, par, gain, plane, line, mine,
    sem_v, sem_d, sem_s, send_h, recv_h, send_c, recv_c, send_n, recv_n,
):
    gx, gy = lax.axis_index("gx"), lax.axis_index("gy")
    up, down = lax.rem(gx + 1, nx), lax.rem(gx + nx - 1, nx)
    right, left = lax.rem(gy + 1, ny), lax.rem(gy + ny - 1, ny)
    groups = cols // 8

    small = [
        pltpu.make_async_copy(region, reg, sem_s.at[0]),
        pltpu.make_async_copy(mask, msk, sem_s.at[1]),
        pltpu.make_async_copy(ws_hbm, ws, sem_s.at[2]),
        pltpu.make_async_copy(wa_hbm, wa, sem_s.at[3]),
        pltpu.make_async_copy(sigma_hbm, sigma, sem_s.at[4]),
        pltpu.make_async_copy(cap_hbm, cap, sem_s.at[5]),
    ]
    for copy in small:
        copy.start()

    def load_row(r, c):
        for zt in range(ZT):
            pltpu.make_async_copy(
                volt.at[r, :, pl.ds(zt * LANES, LANES)],
                v.at[r, zt, pl.ds(PAD, cols), :],
                sem_v.at[r],
            ).start()
        pltpu.make_async_copy(drive.at[r], dr.at[r], sem_d.at[r]).start()
        return c

    lax.fori_loop(0, rows, load_row, 0)

    depth = nx // INNER
    gz, gi = gx // INNER, lax.rem(gx, INNER)
    base = gx - gi
    near_i = [gi] + [lax.rem(gi + i, INNER) for i in range(1, INNER)]
    near_y = [gy] + [lax.rem(gy + i, ny) for i in range(1, ny)]
    in_plane = [
        {"gx": base + near_i[i], "gy": near_y[k]} for k in range(ny) for i in range(INNER) if i or k
    ]
    in_line = [{"gx": lax.rem(gx + INNER * i, nx)} for i in range(1, depth)]

    barrier = pltpu.get_barrier_semaphore()

    def greet(where):
        pl.semaphore_signal(barrier, inc=1, device_id=where, device_id_type=MESH)

    for where in in_plane + in_line:
        greet(where)

    @pl.when(gi == INNER - 1)
    def _():
        greet({"gx": up})

    @pl.when(gi == 0)
    def _():
        greet({"gx": down})

    partners = len(in_plane) + len(in_line) + (gi == 0).astype(jnp.int32) + (gi == INNER - 1).astype(jnp.int32)

    def wait_volt(r):
        whole = v.at[r, :, pl.ds(PAD, cols), :]
        pltpu.make_async_copy(whole, whole, sem_v.at[r]).wait()

    def remote(src, dst, ssem, rsem, where):
        return pltpu.make_async_remote_copy(
            src_ref=src, dst_ref=dst, send_sem=ssem, recv_sem=rsem,
            device_id=where, device_id_type=MESH,
        )

    piece = cols // CHUNKS
    col_copies = [
        remote(volt.at[:, pl.ds(cols - 1, 1), :], col_l, send_c.at[0], recv_c.at[0], {"gy": right}),
        remote(par.at[:, 4, pl.ds(cols - 1, 1), :], con_l, send_c.at[1], recv_c.at[1], {"gy": right}),
        remote(volt.at[:, pl.ds(0, 1), :], col_r, send_c.at[2], recv_c.at[2], {"gy": left}),
        remote(par.at[:, 4, pl.ds(0, 1), :], con_r, send_c.at[3], recv_c.at[3], {"gy": left}),
    ]
    reg_copies = [
        remote(region.at[rows - 1], reg_p, send_h.at[0, CHUNKS], recv_h.at[0, CHUNKS], {"gx": up}),
        remote(region.at[0], reg_n, send_h.at[1, CHUNKS], recv_h.at[1, CHUNKS], {"gx": down}),
    ]
    row_copies = []
    for k in range(CHUNKS):
        part = pl.ds(k * piece, piece)
        row_copies.append((
            remote(volt.at[rows - 1, part, :], halo_p.at[part, :], send_h.at[0, k], recv_h.at[0, k], {"gx": up}),
            remote(volt.at[0, part, :], halo_n.at[part, :], send_h.at[1, k], recv_h.at[1, k], {"gx": down}),
        ))
    sends = reg_copies + col_copies + [copy for pair in row_copies for copy in pair]

    lane = lax.broadcasted_iota(jnp.int32, (8, LANES), 1)
    high = (lane >= KC).astype(jnp.int32)
    coef = lane % KC
    order = (coef % H + 1).astype(F32) * BASE_FREQ
    freq = jnp.where(coef < H, order, -order)
    partner = jnp.where(coef < H, lane + H, lane - H)
    own = [high + 2 * zt for zt in range(ZT)]
    within = [jnp.full((8, LANES), 2 * zt, jnp.int32) for zt in range(ZT)]
    across = [jnp.where(high == 0, 2 * zt - 1 if zt else NZ - 1, 2 * zt + 1) for zt in range(ZT)]
    left_half = lax.broadcasted_iota(jnp.int32, (cols, LANES), 1) < KC

    edge = jnp.zeros((PAD, LANES), F32)

    def clear(r, c):
        for zt in range(ZT):
            v[r, zt, pl.ds(0, PAD), :] = edge
            v[r, zt, pl.ds(cols + PAD, PAD), :] = edge
        return c

    lax.fori_loop(0, rows, clear, 0)
    flux[...] = jnp.zeros_like(flux)
    for zt in range(ZT):
        side[zt, pl.ds(0, PAD), :] = edge

    for i in (0, 1, 4, 5):
        small[i].wait()

    pairs = rows // 2
    pair_lane = lax.broadcasted_iota(jnp.int32, (NZ, LANES), 1)
    layer = lax.broadcasted_iota(jnp.int32, (NZ, LANES), 0)
    pair_regions = [jnp.concatenate([reg[2 * p], reg[2 * p + 1]], axis=1) for p in range(pairs)]
    conduct = [pick(both, sigma) for both in pair_regions]
    for p in range(pairs):
        here = conduct[p]
        beyond = pltpu.roll(conduct[p + 1], cols, 1) if p + 1 < pairs else jnp.zeros_like(here)
        there = jnp.where(pair_lane < cols, pltpu.roll(here, cols, 1), beyond)
        after = jnp.where(pair_lane % cols == cols - 1, 0.0, pltpu.roll(here, LANES - 1, 1))
        deeper = jnp.where(layer == NZ - 1, 0.0, pltpu.roll(here, NZ - 1, 0))
        diode = jnp.concatenate([msk[2 * p], msk[2 * p + 1]], axis=1)
        held_charge = pick(pair_regions[p], cap)
        fields = (
            harmonic_mean(here, there), harmonic_mean(here, after), harmonic_mean(here, deeper),
            jnp.where(diode != 0, -held_charge, held_charge), here,
        )
        for i, field in enumerate(fields):
            flat = widen(jnp.transpose(field))
            par[2 * p, i] = flat[:cols]
            par[2 * p + 1, i] = flat[cols:]
    small[2].wait()
    small[3].wait()

    def pairs_of(r):
        for zt in range(ZT):
            value = v[r, zt, pl.ds(PAD, cols), :]
            other = pltpu.roll(value, KC, 1)
            rest = value - value.astype(BF16).astype(F32)
            other_rest = other - other.astype(BF16).astype(F32)
            x[pl.ds(zt * cols, cols), :] = jnp.where(left_half, value, other_rest).astype(BF16)
            x[pl.ds((ZT + zt) * cols, cols), :] = jnp.where(left_half, other, rest).astype(BF16)
            turned[zt] = other

    def linear(r):
        after = jnp.minimum(r + 1, rows - 1)
        for zt in range(ZT):
            lanes = pl.ds(zt * LANES, LANES)

            def gains(i, index):
                return [spread(par[r, i, pl.ds(8 * j, 8), :], index) for j in range(groups)]

            g_row, g_next, charge = gains(0, own[zt]), gains(1, own[zt]), gains(3, own[zt])
            g_in, g_out = gains(2, within[zt]), gains(2, across[zt])
            for j in range(groups):
                spot = pl.ds(8 * j, 8)
                value = v[r, zt, pl.ds(PAD + 8 * j, 8), :]
                flow = g_row[j] * (value - v[after, zt, pl.ds(PAD + 8 * j, 8), :])
                total = flow - flux[spot, lanes] - dr[r, spot, lanes]
                flux[spot, lanes] = flow
                flow = g_next[j] * (value - v[r, zt, pl.ds(PAD + 8 * j + 1, 8), :])
                side[zt, pl.ds(PAD + 8 * j, 8), :] = flow
                total += flow - side[zt, pl.ds(PAD + 8 * j - 1, 8), :]
                total += g_in[j] * (value - turned[zt, spot, :])
                outer = jnp.where(high == 0, turned[max(zt - 1, 0), spot, :], turned[min(zt + 1, ZT - 1), spot, :])
                total += g_out[j] * (value - outer)
                total += jnp.abs(charge[j]) * (freq * spread(value, partner))
                total += jnp.where(charge[j] < 0.0, 0.5 * value + nl[pl.ds(zt * cols + 8 * j, 8), :], 0.0)
                out[r, spot, lanes] = total

    wait_volt(0)
    pairs_of(0)

    def one_row(r, c):
        @pl.when(r == SEND_AT)
        def _():
            pl.semaphore_wait(barrier, partners)
            for copy in sends:
                copy.start()

        @pl.when(r < rows - 1)
        def _():
            wait_volt(r + 1)

        pltpu.make_async_copy(dr.at[r], dr.at[r], sem_d.at[r]).wait()
        xs = x[...]
        s[...] = jnp.dot(jnp.concatenate([xs, xs], axis=1), ws[...], preferred_element_type=F32)
        for zt in range(ZT):
            for half in range(2):
                wave = s[pl.ds((half * ZT + zt) * cols, cols), :]
                bent = jnp.tanh(wave)
                soft = jnp.abs(wave) - jnp.log(1.0 + jnp.abs(bent))
                y[pl.ds(zt * cols, cols), pl.ds(half * 2 * S, S)] = soft.astype(BF16)
                y[pl.ds(zt * cols, cols), pl.ds(half * 2 * S + S, S)] = bent.astype(BF16)
        full = jnp.dot(y[...], wa[...], preferred_element_type=F32)
        nl[...] = full[:, :LANES] + full[:, LANES:]
        linear(r)
        pairs_of(jnp.minimum(r + 1, rows - 1))
        return c

    lax.fori_loop(0, rows, one_row, 0)

    for copy in col_copies:
        copy.wait_recv()
    sub = lax.broadcasted_iota(jnp.int32, (8, LANES), 0)

    def fix_cols(r, acc):
        first = par[r, 4, pl.ds(0, 8), :]
        last = par[r, 4, pl.ds(cols - 8, 8), :]
        before = jnp.broadcast_to(con_l[r], (8, LANES))
        behind = jnp.broadcast_to(con_r[r], (8, LANES))
        g_l = jnp.where((sub == 0) & (lane < NZ) & (gy > 0), harmonic_mean(first, before), 0.0)
        g_r = jnp.where((sub == 7) & (lane < NZ) & (gy < ny - 1), harmonic_mean(last, behind), 0.0)
        for zt in range(ZT):
            lanes = pl.ds(zt * LANES, LANES)
            out[r, pl.ds(0, 8), lanes] += spread(g_l, own[zt]) * (
                v[r, zt, pl.ds(PAD, 8), :] - jnp.broadcast_to(col_l[r, :, lanes], (8, LANES))
            )
            out[r, pl.ds(cols - 8, 8), lanes] += spread(g_r, own[zt]) * (
                v[r, zt, pl.ds(PAD + cols - 8, 8), :] - jnp.broadcast_to(col_r[r, :, lanes], (8, LANES))
            )
        inner = jnp.where((r > 0) & (r < rows - 1), 1.0, 0.0)
        parts = [jnp.zeros((8, LANES), F32) for _ in range(8)]
        for zt in range(ZT):
            for j in range(groups):
                value = out[r, pl.ds(8 * j, 8), pl.ds(zt * LANES, LANES)]
                parts[j % 8] = parts[j % 8] + value * value
        while len(parts) > 1:
            parts = [a + b for a, b in zip(parts[::2], parts[1::2])]
        return acc + inner * parts[0]

    acc = lax.fori_loop(0, rows, fix_cols, jnp.zeros((8, LANES), F32))

    for end, (copy, marks, r) in enumerate(zip(reg_copies, (reg_p, reg_n), (0, rows - 1))):
        copy.wait_recv()
        field = jnp.concatenate([pick(marks[...], sigma), jnp.zeros((NZ, LANES - cols), F32)], axis=1)
        flat = widen(jnp.transpose(field))[:cols]
        inside = lax.broadcasted_iota(jnp.int32, (cols, LANES), 1) < NZ
        gain[end] = jnp.where(inside, harmonic_mean(par[r, 4], flat), 0.0)
    for k in range(CHUNKS):
        for end, (copy, halo, r) in enumerate(zip(row_copies[k], (halo_p, halo_n), (0, rows - 1))):
            copy.wait_recv()
            parts = [jnp.zeros((8, LANES), F32) for _ in range(8)]
            for j in range(k * piece // 8, (k + 1) * piece // 8):
                spot = pl.ds(8 * j, 8)
                for zt in range(ZT):
                    lanes = pl.ds(zt * LANES, LANES)
                    value = out[r, spot, lanes] + spread(gain[end, spot, :], own[zt]) * (
                        v[r, zt, pl.ds(8 * j + PAD, 8), :] - halo[spot, lanes]
                    )
                    out[r, spot, lanes] = value
                    parts[zt % 8] = parts[zt % 8] + value * value
            while len(parts) > 1:
                parts = [a + b for a, b in zip(parts[::2], parts[1::2])]
            acc = acc + parts[0]

    local = jnp.sum(acc, axis=0, keepdims=True)

    def reduce_over(others, here, value, buf, slot):
        mine[slot] = value
        spot = buf.at[pl.ds(here, 1), :]
        buf[pl.ds(here, 1), :] = value
        for where in others:
            remote(mine.at[slot], spot, send_n.at[slot], recv_n.at[slot], where).start()
        rest = buf.at[pl.ds(0, len(others)), :]
        pltpu.make_async_copy(rest, rest, recv_n.at[slot]).wait()
        return jnp.sum(buf[...], axis=0, keepdims=True)

    value = local + pltpu.roll(local, KC, 1)
    value = reduce_over(in_plane, gy * INNER + gi, value, plane, 0)
    value = reduce_over(in_line, gz, value, line, 1)
    norms[...] = jnp.sqrt(value / cells + NORM_EPS)[0, :KC]

    for slot, buf in enumerate((plane, line)):
        others = buf.at[pl.ds(0, buf.shape[0] - 1), :]
        pltpu.make_async_copy(others, others, send_n.at[slot]).wait()
    for copy in sends:
        copy.wait_send()


def body(nx, ny, volt, drive, region, diode_mask, sigma_table, cap_table):
    rows, cols, width = volt.shape
    cells = rows * cols * NZ * nx * ny
    ws, wa = spectral_tables()
    hbm = pl.BlockSpec(memory_space=pltpu.HBM)
    vmem = pl.BlockSpec(memory_space=pltpu.VMEM)
    dma = pltpu.SemaphoreType.DMA
    held = functools.partial(pltpu.with_memory_space_constraint, memory_space=pltpu.HBM)
    return pl.pallas_call(
        functools.partial(kernel, nx, ny, rows, cols, cells),
        out_shape=(
            jax.ShapeDtypeStruct((rows, cols, width), F32),
            jax.ShapeDtypeStruct((KC,), F32),
        ),
        in_specs=[hbm] * 8,
        out_specs=(vmem, vmem),
        scratch_shapes=[
            pltpu.SMEM((REGIONS,), F32),
            pltpu.SMEM((REGIONS,), F32),
            pltpu.VMEM((rows, ZT, cols + 2 * PAD, LANES), F32),
            pltpu.VMEM((rows, cols, width), F32),
            pltpu.VMEM((rows, NZ, cols), jnp.int32),
            pltpu.VMEM((rows, NZ, cols), jnp.int32),
            pltpu.VMEM(ws.shape, BF16),
            pltpu.VMEM(wa.shape, BF16),
            pltpu.VMEM((cols, width), F32),
            pltpu.VMEM((cols, width), F32),
            pltpu.VMEM((NZ, cols), jnp.int32),
            pltpu.VMEM((NZ, cols), jnp.int32),
            pltpu.VMEM((rows, 1, width), F32),
            pltpu.VMEM((rows, 1, width), F32),
            pltpu.VMEM((rows, 1, LANES), F32),
            pltpu.VMEM((rows, 1, LANES), F32),
            pltpu.VMEM((2 * ZT * cols, LANES), BF16),
            pltpu.VMEM((2 * ZT * cols, S), F32),
            pltpu.VMEM((ZT * cols, 4 * S), BF16),
            pltpu.VMEM((ZT * cols, LANES), F32),
            pltpu.VMEM((cols, width), F32),
            pltpu.VMEM((ZT, cols + PAD, LANES), F32),
            pltpu.VMEM((ZT, cols, LANES), F32),
            pltpu.VMEM((rows, 5, cols, LANES), F32),
            pltpu.VMEM((2, cols, LANES), F32),
            pltpu.VMEM((ny * INNER, LANES), F32),
            pltpu.VMEM((nx // INNER, LANES), F32),
            pltpu.VMEM((2, 1, LANES), F32),
            dma((rows,)), dma((rows,)), dma((6,)),
            dma((2, CHUNKS + 1)), dma((2, CHUNKS + 1)),
            dma((4,)), dma((4,)),
            dma((2,)), dma((2,)),
        ],
        compiler_params=pltpu.CompilerParams(
            collective_id=0, has_side_effects=True, vmem_limit_bytes=38 * 1024 * 1024
        ),
        name="residual",
    )(
        held(volt), held(drive), held(jnp.swapaxes(region, 1, 2)), held(jnp.swapaxes(diode_mask, 1, 2)),
        held(sigma_table), held(cap_table), held(ws), held(wa),
    )


def solution(mesh):
    nx, ny = mesh.shape["gx"], mesh.shape["gy"]
    cut = P("gx", "gy", None)
    return jax.shard_map(
        functools.partial(body, nx, ny), mesh=mesh, in_specs=(cut, cut, cut, cut, P(), P()),
        out_specs=(cut, P()), check_vma=False,
    )
```

```python
import functools
import math

import jax
import jax.numpy as jnp
import numpy as np
from jax import lax
from jax.experimental import pallas as pl
from jax.experimental.pallas import tpu as pltpu
from jax.sharding import PartitionSpec as P

NZ = 32
H = 32
KC = 64
S = 256
REGIONS = 8
BASE_FREQ = 0.1
NORM_EPS = 1e-06
LANES = 128
ZT = NZ * KC // LANES
INNER = 4
PAD = 8
CHUNKS = 2
SEND_AT = 0

MESH = pl.DeviceIdType.MESH
F32 = jnp.float32
BF16 = jnp.bfloat16


def split(table):
    high = table.astype(jnp.bfloat16)
    low = (table - high.astype(np.float64)).astype(jnp.bfloat16)
    return high, low


def spectral_tables():
    orders = np.arange(1, H + 1, dtype=np.float64)
    steps = np.arange(S, dtype=np.int64)
    angles = 2.0 * math.pi * ((orders[:, None].astype(np.int64) * steps[None, :]) % S) / S
    cosines, sines = np.cos(angles), np.sin(angles)
    synthesis = np.concatenate([cosines, sines], axis=0)
    analysis = synthesis.T * (2.0 / S)
    freq = BASE_FREQ * orders
    derived = np.concatenate([freq * analysis[:, H:], -freq * analysis[:, :H]], axis=1)
    high, low = split(synthesis)
    ws = np.concatenate([high, high, low, low], axis=0)
    both = 0.5 * np.concatenate([analysis, derived], axis=0)
    high, low = split(both)
    wa = np.zeros((2, 2 * S, 2, LANES), jnp.bfloat16)
    for half in range(2):
        wa[half, :, 0, half * KC : half * KC + KC] = high
        wa[half, :, 1, half * KC : half * KC + KC] = low
    return ws, wa.reshape(4 * S, 2 * LANES)


def harmonic_mean(left, right):
    return 2.0 * left * right / (left + right)


def pick(region, table):
    value = jnp.full(region.shape, table[0], F32)
    for idx in range(1, REGIONS):
        value = jnp.where(region == idx, table[idx], value)
    return value


def widen(compact):
    rows, count = compact.shape
    return jnp.concatenate([compact, jnp.zeros((rows, LANES - count), compact.dtype)], axis=1)


def spread(compact, index):
    return jnp.take_along_axis(compact, index, axis=1, mode="promise_in_bounds")


def kernel(
    nx, ny, rows, cols, cells,
    volt, drive, region, mask, sigma_hbm, cap_hbm, ws_hbm, wa_hbm,
    out, norms,
    sigma, cap, v, dr, reg, msk, ws, wa,
    halo_p, halo_n, reg_p, reg_n, col_l, col_r, con_l, con_r,
    x, s, y, nl, flux, side, turned, par, gain, plane, line, mine,
    sem_v, sem_d, sem_s, send_h, recv_h, send_c, recv_c, send_n, recv_n,
):
    gx, gy = lax.axis_index("gx"), lax.axis_index("gy")
    up, down = lax.rem(gx + 1, nx), lax.rem(gx + nx - 1, nx)
    right, left = lax.rem(gy + 1, ny), lax.rem(gy + ny - 1, ny)
    groups = cols // 8

    small = [
        pltpu.make_async_copy(region, reg, sem_s.at[0]),
        pltpu.make_async_copy(mask, msk, sem_s.at[1]),
        pltpu.make_async_copy(ws_hbm, ws, sem_s.at[2]),
        pltpu.make_async_copy(wa_hbm, wa, sem_s.at[3]),
        pltpu.make_async_copy(sigma_hbm, sigma, sem_s.at[4]),
        pltpu.make_async_copy(cap_hbm, cap, sem_s.at[5]),
    ]
    for copy in small:
        copy.start()

    def load_row(r, c):
        for zt in range(ZT):
            pltpu.make_async_copy(
                volt.at[r, :, pl.ds(zt * LANES, LANES)],
                v.at[r, zt, pl.ds(PAD, cols), :],
                sem_v.at[r],
            ).start()
        pltpu.make_async_copy(drive.at[r], dr.at[r], sem_d.at[r]).start()
        return c

    lax.fori_loop(0, rows, load_row, 0)

    depth = nx // INNER
    gz, gi = gx // INNER, lax.rem(gx, INNER)
    base = gx - gi
    near_i = [gi] + [lax.rem(gi + i, INNER) for i in range(1, INNER)]
    near_y = [gy] + [lax.rem(gy + i, ny) for i in range(1, ny)]
    in_plane = [
        {"gx": base + near_i[i], "gy": near_y[k]} for k in range(ny) for i in range(INNER) if i or k
    ]
    in_line = [{"gx": lax.rem(gx + INNER * i, nx)} for i in range(1, depth)]

    barrier = pltpu.get_barrier_semaphore()

    def greet(where):
        pl.semaphore_signal(barrier, inc=1, device_id=where, device_id_type=MESH)

    for where in in_plane + in_line:
        greet(where)

    @pl.when(gi == INNER - 1)
    def _():
        greet({"gx": up})

    @pl.when(gi == 0)
    def _():
        greet({"gx": down})

    partners = len(in_plane) + len(in_line) + (gi == 0).astype(jnp.int32) + (gi == INNER - 1).astype(jnp.int32)

    def wait_volt(r):
        whole = v.at[r, :, pl.ds(PAD, cols), :]
        pltpu.make_async_copy(whole, whole, sem_v.at[r]).wait()

    def remote(src, dst, ssem, rsem, where):
        return pltpu.make_async_remote_copy(
            src_ref=src, dst_ref=dst, send_sem=ssem, recv_sem=rsem,
            device_id=where, device_id_type=MESH,
        )

    piece = cols // CHUNKS
    col_copies = [
        remote(volt.at[:, pl.ds(cols - 1, 1), :], col_l, send_c.at[0], recv_c.at[0], {"gy": right}),
        remote(par.at[:, 4, pl.ds(cols - 1, 1), :], con_l, send_c.at[1], recv_c.at[1], {"gy": right}),
        remote(volt.at[:, pl.ds(0, 1), :], col_r, send_c.at[2], recv_c.at[2], {"gy": left}),
        remote(par.at[:, 4, pl.ds(0, 1), :], con_r, send_c.at[3], recv_c.at[3], {"gy": left}),
    ]
    reg_copies = [
        remote(region.at[rows - 1], reg_p, send_h.at[0, CHUNKS], recv_h.at[0, CHUNKS], {"gx": up}),
        remote(region.at[0], reg_n, send_h.at[1, CHUNKS], recv_h.at[1, CHUNKS], {"gx": down}),
    ]
    row_copies = []
    for k in range(CHUNKS):
        part = pl.ds(k * piece, piece)
        row_copies.append((
            remote(volt.at[rows - 1, part, :], halo_p.at[part, :], send_h.at[0, k], recv_h.at[0, k], {"gx": up}),
            remote(volt.at[0, part, :], halo_n.at[part, :], send_h.at[1, k], recv_h.at[1, k], {"gx": down}),
        ))
    sends = reg_copies + col_copies + [copy for pair in row_copies for copy in pair]

    lane = lax.broadcasted_iota(jnp.int32, (8, LANES), 1)
    high = (lane >= KC).astype(jnp.int32)
    coef = lane % KC
    order = (coef % H + 1).astype(F32) * BASE_FREQ
    freq = jnp.where(coef < H, order, -order)
    partner = jnp.where(coef < H, lane + H, lane - H)
    own = [high + 2 * zt for zt in range(ZT)]
    within = [jnp.full((8, LANES), 2 * zt, jnp.int32) for zt in range(ZT)]
    across = [jnp.where(high == 0, 2 * zt - 1 if zt else NZ - 1, 2 * zt + 1) for zt in range(ZT)]
    left_half = lax.broadcasted_iota(jnp.int32, (cols, LANES), 1) < KC

    edge = jnp.zeros((PAD, LANES), F32)

    def clear(r, c):
        for zt in range(ZT):
            v[r, zt, pl.ds(0, PAD), :] = edge
            v[r, zt, pl.ds(cols + PAD, PAD), :] = edge
        return c

    lax.fori_loop(0, rows, clear, 0)
    flux[...] = jnp.zeros_like(flux)
    for zt in range(ZT):
        side[zt, pl.ds(0, PAD), :] = edge

    for copy in small:
        copy.wait()
    wait_volt(0)

    def pairs_of(r):
        for zt in range(ZT):
            value = v[r, zt, pl.ds(PAD, cols), :]
            other = pltpu.roll(value, KC, 1)
            rest = value - value.astype(BF16).astype(F32)
            other_rest = other - other.astype(BF16).astype(F32)
            x[pl.ds(zt * cols, cols), :] = jnp.where(left_half, value, other_rest).astype(BF16)
            x[pl.ds((ZT + zt) * cols, cols), :] = jnp.where(left_half, other, rest).astype(BF16)
            turned[zt] = other

    pairs_of(0)

    pairs = rows // 2
    pair_lane = lax.broadcasted_iota(jnp.int32, (NZ, LANES), 1)
    layer = lax.broadcasted_iota(jnp.int32, (NZ, LANES), 0)
    pair_regions = [jnp.concatenate([reg[2 * p], reg[2 * p + 1]], axis=1) for p in range(pairs)]
    conduct = [pick(both, sigma) for both in pair_regions]
    for p in range(pairs):
        here = conduct[p]
        beyond = pltpu.roll(conduct[p + 1], cols, 1) if p + 1 < pairs else jnp.zeros_like(here)
        there = jnp.where(pair_lane < cols, pltpu.roll(here, cols, 1), beyond)
        after = jnp.where(pair_lane % cols == cols - 1, 0.0, pltpu.roll(here, LANES - 1, 1))
        deeper = jnp.where(layer == NZ - 1, 0.0, pltpu.roll(here, NZ - 1, 0))
        diode = jnp.concatenate([msk[2 * p], msk[2 * p + 1]], axis=1)
        held_charge = pick(pair_regions[p], cap)
        fields = (
            harmonic_mean(here, there), harmonic_mean(here, after), harmonic_mean(here, deeper),
            jnp.where(diode != 0, -held_charge, held_charge), here,
        )
        for i, field in enumerate(fields):
            flat = widen(jnp.transpose(field))
            par[2 * p, i] = flat[:cols]
            par[2 * p + 1, i] = flat[cols:]

    def linear(r):
        after = jnp.minimum(r + 1, rows - 1)
        for zt in range(ZT):
            lanes = pl.ds(zt * LANES, LANES)

            def gains(i, index):
                return [spread(par[r, i, pl.ds(8 * j, 8), :], index) for j in range(groups)]

            g_row, g_next, charge = gains(0, own[zt]), gains(1, own[zt]), gains(3, own[zt])
            g_in, g_out = gains(2, within[zt]), gains(2, across[zt])
            for j in range(groups):
                spot = pl.ds(8 * j, 8)
                value = v[r, zt, pl.ds(PAD + 8 * j, 8), :]
                flow = g_row[j] * (value - v[after, zt, pl.ds(PAD + 8 * j, 8), :])
                total = flow - flux[spot, lanes] - dr[r, spot, lanes]
                flux[spot, lanes] = flow
                flow = g_next[j] * (value - v[r, zt, pl.ds(PAD + 8 * j + 1, 8), :])
                side[zt, pl.ds(PAD + 8 * j, 8), :] = flow
                total += flow - side[zt, pl.ds(PAD + 8 * j - 1, 8), :]
                total += g_in[j] * (value - turned[zt, spot, :])
                outer = jnp.where(high == 0, turned[max(zt - 1, 0), spot, :], turned[min(zt + 1, ZT - 1), spot, :])
                total += g_out[j] * (value - outer)
                total += jnp.abs(charge[j]) * (freq * spread(value, partner))
                total += jnp.where(charge[j] < 0.0, 0.5 * value + nl[pl.ds(zt * cols + 8 * j, 8), :], 0.0)
                out[r, spot, lanes] = total


    def one_row(r, c):
        @pl.when(r == SEND_AT)
        def _():
            pl.semaphore_wait(barrier, partners)
            for copy in sends:
                copy.start()

        @pl.when(r < rows - 1)
        def _():
            wait_volt(r + 1)

        pltpu.make_async_copy(dr.at[r], dr.at[r], sem_d.at[r]).wait()
        xs = x[...]
        s[...] = jnp.dot(jnp.concatenate([xs, xs], axis=1), ws[...], preferred_element_type=F32)
        for zt in range(ZT):
            for half in range(2):
                wave = s[pl.ds((half * ZT + zt) * cols, cols), :]
                bent = jnp.tanh(wave)
                soft = jnp.abs(wave) - jnp.log(1.0 + jnp.abs(bent))
                y[pl.ds(zt * cols, cols), pl.ds(half * 2 * S, S)] = soft.astype(BF16)
                y[pl.ds(zt * cols, cols), pl.ds(half * 2 * S + S, S)] = bent.astype(BF16)
        full = jnp.dot(y[...], wa[...], preferred_element_type=F32)
        nl[...] = full[:, :LANES] + full[:, LANES:]
        linear(r)
        pairs_of(jnp.minimum(r + 1, rows - 1))
        return c

    lax.fori_loop(0, rows, one_row, 0)

    for copy in col_copies:
        copy.wait_recv()
    sub = lax.broadcasted_iota(jnp.int32, (8, LANES), 0)

    def fix_cols(r, acc):
        first = par[r, 4, pl.ds(0, 8), :]
        last = par[r, 4, pl.ds(cols - 8, 8), :]
        before = jnp.broadcast_to(con_l[r], (8, LANES))
        behind = jnp.broadcast_to(con_r[r], (8, LANES))
        g_l = jnp.where((sub == 0) & (lane < NZ) & (gy > 0), harmonic_mean(first, before), 0.0)
        g_r = jnp.where((sub == 7) & (lane < NZ) & (gy < ny - 1), harmonic_mean(last, behind), 0.0)
        for zt in range(ZT):
            lanes = pl.ds(zt * LANES, LANES)
            out[r, pl.ds(0, 8), lanes] += spread(g_l, own[zt]) * (
                v[r, zt, pl.ds(PAD, 8), :] - jnp.broadcast_to(col_l[r, :, lanes], (8, LANES))
            )
            out[r, pl.ds(cols - 8, 8), lanes] += spread(g_r, own[zt]) * (
                v[r, zt, pl.ds(PAD + cols - 8, 8), :] - jnp.broadcast_to(col_r[r, :, lanes], (8, LANES))
            )
        inner = jnp.where((r > 0) & (r < rows - 1), 1.0, 0.0)
        parts = [jnp.zeros((8, LANES), F32) for _ in range(8)]
        for zt in range(ZT):
            for j in range(groups):
                value = out[r, pl.ds(8 * j, 8), pl.ds(zt * LANES, LANES)]
                parts[j % 8] = parts[j % 8] + value * value
        while len(parts) > 1:
            parts = [a + b for a, b in zip(parts[::2], parts[1::2])]
        return acc + inner * parts[0]

    def fix_some(p, acc):
        for i in range(4):
            acc = fix_cols(4 * p + i, acc)
        return acc

    acc = lax.fori_loop(0, rows // 4, fix_some, jnp.zeros((8, LANES), F32))

    for end, (copy, marks, r) in enumerate(zip(reg_copies, (reg_p, reg_n), (0, rows - 1))):
        copy.wait_recv()
        field = jnp.concatenate([pick(marks[...], sigma), jnp.zeros((NZ, LANES - cols), F32)], axis=1)
        flat = widen(jnp.transpose(field))[:cols]
        inside = lax.broadcasted_iota(jnp.int32, (cols, LANES), 1) < NZ
        gain[end] = jnp.where(inside, harmonic_mean(par[r, 4], flat), 0.0)
    for k in range(CHUNKS):
        for end, (copy, halo, r) in enumerate(zip(row_copies[k], (halo_p, halo_n), (0, rows - 1))):
            copy.wait_recv()
            parts = [jnp.zeros((8, LANES), F32) for _ in range(8)]
            for j in range(k * piece // 8, (k + 1) * piece // 8):
                spot = pl.ds(8 * j, 8)
                for zt in range(ZT):
                    lanes = pl.ds(zt * LANES, LANES)
                    value = out[r, spot, lanes] + spread(gain[end, spot, :], own[zt]) * (
                        v[r, zt, pl.ds(8 * j + PAD, 8), :] - halo[spot, lanes]
                    )
                    out[r, spot, lanes] = value
                    parts[zt % 8] = parts[zt % 8] + value * value
            while len(parts) > 1:
                parts = [a + b for a, b in zip(parts[::2], parts[1::2])]
            acc = acc + parts[0]

    local = jnp.sum(acc, axis=0, keepdims=True)

    def reduce_over(others, here, value, buf, slot):
        mine[slot] = value
        spot = buf.at[pl.ds(here, 1), :]
        buf[pl.ds(here, 1), :] = value
        for where in others:
            remote(mine.at[slot], spot, send_n.at[slot], recv_n.at[slot], where).start()
        rest = buf.at[pl.ds(0, len(others)), :]
        pltpu.make_async_copy(rest, rest, recv_n.at[slot]).wait()
        return jnp.sum(buf[...], axis=0, keepdims=True)

    value = local + pltpu.roll(local, KC, 1)
    value = reduce_over(in_plane, gy * INNER + gi, value, plane, 0)
    value = reduce_over(in_line, gz, value, line, 1)
    norms[...] = jnp.sqrt(value / cells + NORM_EPS)[0, :KC]

    for slot, buf in enumerate((plane, line)):
        others = buf.at[pl.ds(0, buf.shape[0] - 1), :]
        pltpu.make_async_copy(others, others, send_n.at[slot]).wait()
    for copy in sends:
        copy.wait_send()


def write_out(residual, norms, residual_out, norms_out, sems):
    count = residual.shape[0]
    copies = [pltpu.make_async_copy(residual.at[r], residual_out.at[r], sems.at[r]) for r in range(count)]
    copies.append(pltpu.make_async_copy(norms, norms_out, sems.at[count]))
    for copy in copies:
        copy.start()
    for copy in copies:
        copy.wait()


def body(nx, ny, volt, drive, region, diode_mask, sigma_table, cap_table):
    rows, cols, width = volt.shape
    cells = rows * cols * NZ * nx * ny
    ws, wa = spectral_tables()
    hbm = pl.BlockSpec(memory_space=pltpu.HBM)
    vmem = pl.BlockSpec(memory_space=pltpu.VMEM)
    dma = pltpu.SemaphoreType.DMA
    held = functools.partial(pltpu.with_memory_space_constraint, memory_space=pltpu.HBM)
    residual, norms = pl.pallas_call(
        functools.partial(kernel, nx, ny, rows, cols, cells),
        out_shape=(
            jax.ShapeDtypeStruct((rows, cols, width), F32),
            jax.ShapeDtypeStruct((KC,), F32),
        ),
        in_specs=[hbm] * 8,
        out_specs=(vmem, vmem),
        scratch_shapes=[
            pltpu.SMEM((REGIONS,), F32),
            pltpu.SMEM((REGIONS,), F32),
            pltpu.VMEM((rows, ZT, cols + 2 * PAD, LANES), F32),
            pltpu.VMEM((rows, cols, width), F32),
            pltpu.VMEM((rows, NZ, cols), jnp.int32),
            pltpu.VMEM((rows, NZ, cols), jnp.int32),
            pltpu.VMEM(ws.shape, BF16),
            pltpu.VMEM(wa.shape, BF16),
            pltpu.VMEM((cols, width), F32),
            pltpu.VMEM((cols, width), F32),
            pltpu.VMEM((NZ, cols), jnp.int32),
            pltpu.VMEM((NZ, cols), jnp.int32),
            pltpu.VMEM((rows, 1, width), F32),
            pltpu.VMEM((rows, 1, width), F32),
            pltpu.VMEM((rows, 1, LANES), F32),
            pltpu.VMEM((rows, 1, LANES), F32),
            pltpu.VMEM((2 * ZT * cols, LANES), BF16),
            pltpu.VMEM((2 * ZT * cols, S), F32),
            pltpu.VMEM((ZT * cols, 4 * S), BF16),
            pltpu.VMEM((ZT * cols, LANES), F32),
            pltpu.VMEM((cols, width), F32),
            pltpu.VMEM((ZT, cols + PAD, LANES), F32),
            pltpu.VMEM((ZT, cols, LANES), F32),
            pltpu.VMEM((rows, 5, cols, LANES), F32),
            pltpu.VMEM((2, cols, LANES), F32),
            pltpu.VMEM((ny * INNER, LANES), F32),
            pltpu.VMEM((nx // INNER, LANES), F32),
            pltpu.VMEM((2, 1, LANES), F32),
            dma((rows,)), dma((rows,)), dma((6,)),
            dma((2, CHUNKS + 1)), dma((2, CHUNKS + 1)),
            dma((4,)), dma((4,)),
            dma((2,)), dma((2,)),
        ],
        compiler_params=pltpu.CompilerParams(
            collective_id=0, has_side_effects=True, vmem_limit_bytes=38 * 1024 * 1024
        ),
        name="residual",
    )(
        held(volt), held(drive), held(jnp.swapaxes(region, 1, 2)), held(jnp.swapaxes(diode_mask, 1, 2)),
        held(sigma_table), held(cap_table), held(ws), held(wa),
    )
    return pl.pallas_call(
        write_out,
        out_shape=(jax.ShapeDtypeStruct(residual.shape, F32), jax.ShapeDtypeStruct(norms.shape, F32)),
        in_specs=[vmem, vmem],
        out_specs=(hbm, hbm),
        scratch_shapes=[dma((rows + 1,))],
        compiler_params=pltpu.CompilerParams(vmem_limit_bytes=8 * 1024 * 1024),
        name="write_out",
    )(residual, norms)


def solution(mesh):
    nx, ny = mesh.shape["gx"], mesh.shape["gy"]
    cut = P("gx", "gy", None)
    return jax.shard_map(
        functools.partial(body, nx, ny), mesh=mesh, in_specs=(cut, cut, cut, cut, P(), P()),
        out_specs=(cut, P()), check_vma=False,
    )
```

```python
import functools
import math

import jax
import jax.numpy as jnp
import numpy as np
from jax import lax
from jax.experimental import pallas as pl
from jax.experimental.pallas import tpu as pltpu
from jax.sharding import PartitionSpec as P

NZ = 32
H = 32
KC = 64
S = 256
REGIONS = 8
BASE_FREQ = 0.1
NORM_EPS = 1e-06
LANES = 128
ZT = NZ * KC // LANES
INNER = 4
PAD = 8
CHUNKS = 2
SEND_AT = 0

MESH = pl.DeviceIdType.MESH
F32 = jnp.float32
BF16 = jnp.bfloat16


def split(table):
    high = table.astype(jnp.bfloat16)
    low = (table - high.astype(np.float64)).astype(jnp.bfloat16)
    return high, low


def spectral_tables():
    orders = np.arange(1, H + 1, dtype=np.float64)
    steps = np.arange(S, dtype=np.int64)
    angles = 2.0 * math.pi * ((orders[:, None].astype(np.int64) * steps[None, :]) % S) / S
    cosines, sines = np.cos(angles), np.sin(angles)
    synthesis = np.concatenate([cosines, sines], axis=0)
    analysis = synthesis.T * (2.0 / S)
    freq = BASE_FREQ * orders
    derived = np.concatenate([freq * analysis[:, H:], -freq * analysis[:, :H]], axis=1)
    high, low = split(synthesis)
    ws = np.concatenate([high, high, low, low], axis=0)
    both = 0.5 * np.concatenate([analysis, derived], axis=0)
    high, low = split(both)
    wa = np.zeros((2, 2 * S, 2, LANES), jnp.bfloat16)
    for half in range(2):
        wa[half, :, 0, half * KC : half * KC + KC] = high
        wa[half, :, 1, half * KC : half * KC + KC] = low
    return ws, wa.reshape(4 * S, 2 * LANES)


def harmonic_mean(left, right):
    return 2.0 * left * right / (left + right)


def pick(region, table):
    value = jnp.full(region.shape, table[0], F32)
    for idx in range(1, REGIONS):
        value = jnp.where(region == idx, table[idx], value)
    return value


def widen(compact):
    rows, count = compact.shape
    return jnp.concatenate([compact, jnp.zeros((rows, LANES - count), compact.dtype)], axis=1)


def spread(compact, index):
    return jnp.take_along_axis(compact, index, axis=1, mode="promise_in_bounds")


def kernel(
    nx, ny, rows, cols, cells,
    volt, drive, region, mask, sigma_hbm, cap_hbm, ws_hbm, wa_hbm,
    out, norms,
    sigma, cap, v, dr, reg, msk, ws, wa,
    halo_p, halo_n, reg_p, reg_n, col_l, col_r, con_l, con_r,
    x, s, y, nl, flux, side, turned, par, gain, plane, line, mine,
    sem_v, sem_d, sem_s, send_h, recv_h, send_c, recv_c, send_n, recv_n, hello,
):
    gx, gy = lax.axis_index("gx"), lax.axis_index("gy")
    up, down = lax.rem(gx + 1, nx), lax.rem(gx + nx - 1, nx)
    right, left = lax.rem(gy + 1, ny), lax.rem(gy + ny - 1, ny)
    groups = cols // 8

    small = [
        pltpu.make_async_copy(region, reg, sem_s.at[0]),
        pltpu.make_async_copy(mask, msk, sem_s.at[1]),
        pltpu.make_async_copy(ws_hbm, ws, sem_s.at[2]),
        pltpu.make_async_copy(wa_hbm, wa, sem_s.at[3]),
        pltpu.make_async_copy(sigma_hbm, sigma, sem_s.at[4]),
        pltpu.make_async_copy(cap_hbm, cap, sem_s.at[5]),
    ]
    for copy in small:
        copy.start()

    def load_row(r, c):
        for zt in range(ZT):
            pltpu.make_async_copy(
                volt.at[r, :, pl.ds(zt * LANES, LANES)],
                v.at[r, zt, pl.ds(PAD, cols), :],
                sem_v.at[r],
            ).start()
        pltpu.make_async_copy(drive.at[r], dr.at[r], sem_d.at[r]).start()
        return c

    lax.fori_loop(0, rows, load_row, 0)

    depth = nx // INNER
    gz, gi = gx // INNER, lax.rem(gx, INNER)
    base = gx - gi
    near_i = [gi] + [lax.rem(gi + i, INNER) for i in range(1, INNER)]
    near_y = [gy] + [lax.rem(gy + i, ny) for i in range(1, ny)]
    in_plane = [
        {"gx": base + near_i[i], "gy": near_y[k]} for k in range(ny) for i in range(INNER) if i or k
    ]
    in_line = [{"gx": lax.rem(gx + INNER * i, nx)} for i in range(1, depth)]

    def at(along, offset):
        mine_here, count = (gx, nx) if along == "gx" else (gy, ny)
        return {along: lax.rem(mine_here + offset + count, count)}

    beside = [at("gy", sign * i) for i in (1, 2) for sign in (1, -1)]
    near = [at("gx", sign * i) for i in range(1, INNER + 1) for sign in (1, -1)] + beside
    first = [at("gx", INNER), at("gx", -INNER)] + beside
    second = [at("gx", 2 * INNER), at("gx", -2 * INNER), at("gy", 2), at("gy", -2)]
    barrier = pltpu.get_barrier_semaphore()
    for where in near:
        pl.semaphore_signal(barrier, inc=1, device_id=where, device_id_type=MESH)

    def wait_volt(r):
        whole = v.at[r, :, pl.ds(PAD, cols), :]
        pltpu.make_async_copy(whole, whole, sem_v.at[r]).wait()

    def remote(src, dst, ssem, rsem, where):
        return pltpu.make_async_remote_copy(
            src_ref=src, dst_ref=dst, send_sem=ssem, recv_sem=rsem,
            device_id=where, device_id_type=MESH,
        )

    piece = cols // CHUNKS
    col_copies = [
        remote(volt.at[:, pl.ds(cols - 1, 1), :], col_l, send_c.at[0], recv_c.at[0], {"gy": right}),
        remote(par.at[:, 4, pl.ds(cols - 1, 1), :], con_l, send_c.at[1], recv_c.at[1], {"gy": right}),
        remote(volt.at[:, pl.ds(0, 1), :], col_r, send_c.at[2], recv_c.at[2], {"gy": left}),
        remote(par.at[:, 4, pl.ds(0, 1), :], con_r, send_c.at[3], recv_c.at[3], {"gy": left}),
    ]
    reg_copies = [
        remote(region.at[rows - 1], reg_p, send_h.at[0, CHUNKS], recv_h.at[0, CHUNKS], {"gx": up}),
        remote(region.at[0], reg_n, send_h.at[1, CHUNKS], recv_h.at[1, CHUNKS], {"gx": down}),
    ]
    row_copies = []
    for k in range(CHUNKS):
        part = pl.ds(k * piece, piece)
        row_copies.append((
            remote(volt.at[rows - 1, part, :], halo_p.at[part, :], send_h.at[0, k], recv_h.at[0, k], {"gx": up}),
            remote(volt.at[0, part, :], halo_n.at[part, :], send_h.at[1, k], recv_h.at[1, k], {"gx": down}),
        ))
    sends = reg_copies + col_copies + [copy for pair in row_copies for copy in pair]

    lane = lax.broadcasted_iota(jnp.int32, (8, LANES), 1)
    high = (lane >= KC).astype(jnp.int32)
    coef = lane % KC
    order = (coef % H + 1).astype(F32) * BASE_FREQ
    freq = jnp.where(coef < H, order, -order)
    partner = jnp.where(coef < H, lane + H, lane - H)
    own = [high + 2 * zt for zt in range(ZT)]
    within = [jnp.full((8, LANES), 2 * zt, jnp.int32) for zt in range(ZT)]
    across = [jnp.where(high == 0, 2 * zt - 1 if zt else NZ - 1, 2 * zt + 1) for zt in range(ZT)]
    left_half = lax.broadcasted_iota(jnp.int32, (cols, LANES), 1) < KC

    edge = jnp.zeros((PAD, LANES), F32)

    def clear(r, c):
        for zt in range(ZT):
            v[r, zt, pl.ds(0, PAD), :] = edge
            v[r, zt, pl.ds(cols + PAD, PAD), :] = edge
        return c

    lax.fori_loop(0, rows, clear, 0)
    flux[...] = jnp.zeros_like(flux)
    for zt in range(ZT):
        side[zt, pl.ds(0, PAD), :] = edge

    for copy in small:
        copy.wait()
    wait_volt(0)

    def pairs_of(r):
        for zt in range(ZT):
            value = v[r, zt, pl.ds(PAD, cols), :]
            other = pltpu.roll(value, KC, 1)
            rest = value - value.astype(BF16).astype(F32)
            other_rest = other - other.astype(BF16).astype(F32)
            x[pl.ds(zt * cols, cols), :] = jnp.where(left_half, value, other_rest).astype(BF16)
            x[pl.ds((ZT + zt) * cols, cols), :] = jnp.where(left_half, other, rest).astype(BF16)
            turned[zt] = other

    pairs_of(0)

    pairs = rows // 2
    pair_lane = lax.broadcasted_iota(jnp.int32, (NZ, LANES), 1)
    layer = lax.broadcasted_iota(jnp.int32, (NZ, LANES), 0)
    pair_regions = [jnp.concatenate([reg[2 * p], reg[2 * p + 1]], axis=1) for p in range(pairs)]
    conduct = [pick(both, sigma) for both in pair_regions]
    for p in range(pairs):
        here = conduct[p]
        beyond = pltpu.roll(conduct[p + 1], cols, 1) if p + 1 < pairs else jnp.zeros_like(here)
        there = jnp.where(pair_lane < cols, pltpu.roll(here, cols, 1), beyond)
        after = jnp.where(pair_lane % cols == cols - 1, 0.0, pltpu.roll(here, LANES - 1, 1))
        deeper = jnp.where(layer == NZ - 1, 0.0, pltpu.roll(here, NZ - 1, 0))
        diode = jnp.concatenate([msk[2 * p], msk[2 * p + 1]], axis=1)
        held_charge = pick(pair_regions[p], cap)
        fields = (
            harmonic_mean(here, there), harmonic_mean(here, after), harmonic_mean(here, deeper),
            jnp.where(diode != 0, -held_charge, held_charge), here,
        )
        for i, field in enumerate(fields):
            flat = widen(jnp.transpose(field))
            par[2 * p, i] = flat[:cols]
            par[2 * p + 1, i] = flat[cols:]

    def linear(r):
        after = jnp.minimum(r + 1, rows - 1)
        for zt in range(ZT):
            lanes = pl.ds(zt * LANES, LANES)

            def gains(i, index):
                return [spread(par[r, i, pl.ds(8 * j, 8), :], index) for j in range(groups)]

            g_row, g_next, charge = gains(0, own[zt]), gains(1, own[zt]), gains(3, own[zt])
            g_in, g_out = gains(2, within[zt]), gains(2, across[zt])
            for j in range(groups):
                spot = pl.ds(8 * j, 8)
                value = v[r, zt, pl.ds(PAD + 8 * j, 8), :]
                flow = g_row[j] * (value - v[after, zt, pl.ds(PAD + 8 * j, 8), :])
                total = flow - flux[spot, lanes] - dr[r, spot, lanes]
                flux[spot, lanes] = flow
                flow = g_next[j] * (value - v[r, zt, pl.ds(PAD + 8 * j + 1, 8), :])
                side[zt, pl.ds(PAD + 8 * j, 8), :] = flow
                total += flow - side[zt, pl.ds(PAD + 8 * j - 1, 8), :]
                total += g_in[j] * (value - turned[zt, spot, :])
                outer = jnp.where(high == 0, turned[max(zt - 1, 0), spot, :], turned[min(zt + 1, ZT - 1), spot, :])
                total += g_out[j] * (value - outer)
                total += jnp.abs(charge[j]) * (freq * spread(value, partner))
                total += jnp.where(charge[j] < 0.0, 0.5 * value + nl[pl.ds(zt * cols + 8 * j, 8), :], 0.0)
                out[r, spot, lanes] = total


    def one_row(r, c):
        @pl.when(r == SEND_AT)
        def _():
            pl.semaphore_wait(barrier, len(near))
            for copy in sends:
                copy.start()
            for where in first:
                pl.semaphore_signal(hello.at[0], inc=1, device_id=where, device_id_type=MESH)

        @pl.when(r == rows // 2)
        def _():
            pl.semaphore_wait(hello.at[0], len(first))
            for where in second:
                pl.semaphore_signal(hello.at[1], inc=1, device_id=where, device_id_type=MESH)

        @pl.when(r < rows - 1)
        def _():
            wait_volt(r + 1)

        pltpu.make_async_copy(dr.at[r], dr.at[r], sem_d.at[r]).wait()
        xs = x[...]
        s[...] = jnp.dot(jnp.concatenate([xs, xs], axis=1), ws[...], preferred_element_type=F32)
        for zt in range(ZT):
            for half in range(2):
                wave = s[pl.ds((half * ZT + zt) * cols, cols), :]
                bent = jnp.tanh(wave)
                soft = jnp.abs(wave) - jnp.log(1.0 + jnp.abs(bent))
                y[pl.ds(zt * cols, cols), pl.ds(half * 2 * S, S)] = soft.astype(BF16)
                y[pl.ds(zt * cols, cols), pl.ds(half * 2 * S + S, S)] = bent.astype(BF16)
        full = jnp.dot(y[...], wa[...], preferred_element_type=F32)
        nl[...] = full[:, :LANES] + full[:, LANES:]
        linear(r)
        pairs_of(jnp.minimum(r + 1, rows - 1))
        return c

    lax.fori_loop(0, rows, one_row, 0)

    for copy in col_copies:
        copy.wait_recv()
    sub = lax.broadcasted_iota(jnp.int32, (8, LANES), 0)

    def fix_cols(r, acc):
        first = par[r, 4, pl.ds(0, 8), :]
        last = par[r, 4, pl.ds(cols - 8, 8), :]
        before = jnp.broadcast_to(con_l[r], (8, LANES))
        behind = jnp.broadcast_to(con_r[r], (8, LANES))
        g_l = jnp.where((sub == 0) & (lane < NZ) & (gy > 0), harmonic_mean(first, before), 0.0)
        g_r = jnp.where((sub == 7) & (lane < NZ) & (gy < ny - 1), harmonic_mean(last, behind), 0.0)
        for zt in range(ZT):
            lanes = pl.ds(zt * LANES, LANES)
            out[r, pl.ds(0, 8), lanes] += spread(g_l, own[zt]) * (
                v[r, zt, pl.ds(PAD, 8), :] - jnp.broadcast_to(col_l[r, :, lanes], (8, LANES))
            )
            out[r, pl.ds(cols - 8, 8), lanes] += spread(g_r, own[zt]) * (
                v[r, zt, pl.ds(PAD + cols - 8, 8), :] - jnp.broadcast_to(col_r[r, :, lanes], (8, LANES))
            )
        inner = jnp.where((r > 0) & (r < rows - 1), 1.0, 0.0)
        parts = [jnp.zeros((8, LANES), F32) for _ in range(8)]
        for zt in range(ZT):
            for j in range(groups):
                value = out[r, pl.ds(8 * j, 8), pl.ds(zt * LANES, LANES)]
                parts[j % 8] = parts[j % 8] + value * value
        while len(parts) > 1:
            parts = [a + b for a, b in zip(parts[::2], parts[1::2])]
        return acc + inner * parts[0]

    def fix_some(p, acc):
        for i in range(4):
            acc = fix_cols(4 * p + i, acc)
        return acc

    acc = lax.fori_loop(0, rows // 4, fix_some, jnp.zeros((8, LANES), F32))

    for end, (copy, marks, r) in enumerate(zip(reg_copies, (reg_p, reg_n), (0, rows - 1))):
        copy.wait_recv()
        field = jnp.concatenate([pick(marks[...], sigma), jnp.zeros((NZ, LANES - cols), F32)], axis=1)
        flat = widen(jnp.transpose(field))[:cols]
        inside = lax.broadcasted_iota(jnp.int32, (cols, LANES), 1) < NZ
        gain[end] = jnp.where(inside, harmonic_mean(par[r, 4], flat), 0.0)
    for k in range(CHUNKS):
        for end, (copy, halo, r) in enumerate(zip(row_copies[k], (halo_p, halo_n), (0, rows - 1))):
            copy.wait_recv()
            parts = [jnp.zeros((8, LANES), F32) for _ in range(8)]
            for j in range(k * piece // 8, (k + 1) * piece // 8):
                spot = pl.ds(8 * j, 8)
                for zt in range(ZT):
                    lanes = pl.ds(zt * LANES, LANES)
                    value = out[r, spot, lanes] + spread(gain[end, spot, :], own[zt]) * (
                        v[r, zt, pl.ds(8 * j + PAD, 8), :] - halo[spot, lanes]
                    )
                    out[r, spot, lanes] = value
                    parts[zt % 8] = parts[zt % 8] + value * value
            while len(parts) > 1:
                parts = [a + b for a, b in zip(parts[::2], parts[1::2])]
            acc = acc + parts[0]

    local = jnp.sum(acc, axis=0, keepdims=True)
    pl.semaphore_wait(hello.at[1], len(second))

    def reduce_over(others, here, value, buf, slot):
        mine[slot] = value
        spot = buf.at[pl.ds(here, 1), :]
        buf[pl.ds(here, 1), :] = value
        for where in others:
            remote(mine.at[slot], spot, send_n.at[slot], recv_n.at[slot], where).start()
        rest = buf.at[pl.ds(0, len(others)), :]
        pltpu.make_async_copy(rest, rest, recv_n.at[slot]).wait()
        return jnp.sum(buf[...], axis=0, keepdims=True)

    value = local + pltpu.roll(local, KC, 1)
    value = reduce_over(in_plane, gy * INNER + gi, value, plane, 0)
    value = reduce_over(in_line, gz, value, line, 1)
    norms[...] = jnp.sqrt(value / cells + NORM_EPS)[0, :KC]

    for slot, buf in enumerate((plane, line)):
        others = buf.at[pl.ds(0, buf.shape[0] - 1), :]
        pltpu.make_async_copy(others, others, send_n.at[slot]).wait()
    for copy in sends:
        copy.wait_send()


def write_out(residual, norms, residual_out, norms_out, sems):
    count = residual.shape[0]
    copies = [pltpu.make_async_copy(residual.at[r], residual_out.at[r], sems.at[r]) for r in range(count)]
    copies.append(pltpu.make_async_copy(norms, norms_out, sems.at[count]))
    for copy in copies:
        copy.start()
    for copy in copies:
        copy.wait()


def body(nx, ny, volt, drive, region, diode_mask, sigma_table, cap_table):
    rows, cols, width = volt.shape
    cells = rows * cols * NZ * nx * ny
    ws, wa = spectral_tables()
    hbm = pl.BlockSpec(memory_space=pltpu.HBM)
    vmem = pl.BlockSpec(memory_space=pltpu.VMEM)
    dma = pltpu.SemaphoreType.DMA
    held = functools.partial(pltpu.with_memory_space_constraint, memory_space=pltpu.HBM)
    residual, norms = pl.pallas_call(
        functools.partial(kernel, nx, ny, rows, cols, cells),
        out_shape=(
            jax.ShapeDtypeStruct((rows, cols, width), F32),
            jax.ShapeDtypeStruct((KC,), F32),
        ),
        in_specs=[hbm] * 8,
        out_specs=(vmem, vmem),
        scratch_shapes=[
            pltpu.SMEM((REGIONS,), F32),
            pltpu.SMEM((REGIONS,), F32),
            pltpu.VMEM((rows, ZT, cols + 2 * PAD, LANES), F32),
            pltpu.VMEM((rows, cols, width), F32),
            pltpu.VMEM((rows, NZ, cols), jnp.int32),
            pltpu.VMEM((rows, NZ, cols), jnp.int32),
            pltpu.VMEM(ws.shape, BF16),
            pltpu.VMEM(wa.shape, BF16),
            pltpu.VMEM((cols, width), F32),
            pltpu.VMEM((cols, width), F32),
            pltpu.VMEM((NZ, cols), jnp.int32),
            pltpu.VMEM((NZ, cols), jnp.int32),
            pltpu.VMEM((rows, 1, width), F32),
            pltpu.VMEM((rows, 1, width), F32),
            pltpu.VMEM((rows, 1, LANES), F32),
            pltpu.VMEM((rows, 1, LANES), F32),
            pltpu.VMEM((2 * ZT * cols, LANES), BF16),
            pltpu.VMEM((2 * ZT * cols, S), F32),
            pltpu.VMEM((ZT * cols, 4 * S), BF16),
            pltpu.VMEM((ZT * cols, LANES), F32),
            pltpu.VMEM((cols, width), F32),
            pltpu.VMEM((ZT, cols + PAD, LANES), F32),
            pltpu.VMEM((ZT, cols, LANES), F32),
            pltpu.VMEM((rows, 5, cols, LANES), F32),
            pltpu.VMEM((2, cols, LANES), F32),
            pltpu.VMEM((ny * INNER, LANES), F32),
            pltpu.VMEM((nx // INNER, LANES), F32),
            pltpu.VMEM((2, 1, LANES), F32),
            dma((rows,)), dma((rows,)), dma((6,)),
            dma((2, CHUNKS + 1)), dma((2, CHUNKS + 1)),
            dma((4,)), dma((4,)),
            dma((2,)), dma((2,)), pltpu.SemaphoreType.REGULAR((2,)),
        ],
        compiler_params=pltpu.CompilerParams(
            collective_id=0, has_side_effects=True, vmem_limit_bytes=38 * 1024 * 1024
        ),
        name="residual",
    )(
        held(volt), held(drive), held(jnp.swapaxes(region, 1, 2)), held(jnp.swapaxes(diode_mask, 1, 2)),
        held(sigma_table), held(cap_table), held(ws), held(wa),
    )
    return pl.pallas_call(
        write_out,
        out_shape=(jax.ShapeDtypeStruct(residual.shape, F32), jax.ShapeDtypeStruct(norms.shape, F32)),
        in_specs=[vmem, vmem],
        out_specs=(hbm, hbm),
        scratch_shapes=[dma((rows + 1,))],
        compiler_params=pltpu.CompilerParams(vmem_limit_bytes=8 * 1024 * 1024),
        name="write_out",
    )(residual, norms)


def solution(mesh):
    nx, ny = mesh.shape["gx"], mesh.shape["gy"]
    cut = P("gx", "gy", None)
    return jax.shard_map(
        functools.partial(body, nx, ny), mesh=mesh, in_specs=(cut, cut, cut, cut, P(), P()),
        out_specs=(cut, P()), check_vma=False,
    )
```

```python
import functools
import math

import jax
import jax.numpy as jnp
import numpy as np
from jax import lax
from jax.experimental import pallas as pl
from jax.experimental.pallas import tpu as pltpu
from jax.sharding import PartitionSpec as P

NZ = 32
H = 32
KC = 64
S = 256
REGIONS = 8
BASE_FREQ = 0.1
NORM_EPS = 1e-06
LANES = 128
ZT = NZ * KC // LANES
INNER = 4
PAD = 8
CHUNKS = 4
SEND_AT = 0

MESH = pl.DeviceIdType.MESH
F32 = jnp.float32
BF16 = jnp.bfloat16


def split(table):
    high = table.astype(jnp.bfloat16)
    low = (table - high.astype(np.float64)).astype(jnp.bfloat16)
    return high, low


def spectral_tables():
    orders = np.arange(1, H + 1, dtype=np.float64)
    steps = np.arange(S, dtype=np.int64)
    angles = 2.0 * math.pi * ((orders[:, None].astype(np.int64) * steps[None, :]) % S) / S
    cosines, sines = np.cos(angles), np.sin(angles)
    synthesis = np.concatenate([cosines, sines], axis=0)
    analysis = synthesis.T * (2.0 / S)
    freq = BASE_FREQ * orders
    derived = np.concatenate([freq * analysis[:, H:], -freq * analysis[:, :H]], axis=1)
    high, low = split(synthesis)
    ws = np.concatenate([high, high, low, low], axis=0)
    both = 0.5 * np.concatenate([analysis, derived], axis=0)
    high, low = split(both)
    wa = np.zeros((2, 2 * S, 2, LANES), jnp.bfloat16)
    for half in range(2):
        wa[half, :, 0, half * KC : half * KC + KC] = high
        wa[half, :, 1, half * KC : half * KC + KC] = low
    return ws, wa.reshape(4 * S, 2 * LANES)


def harmonic_mean(left, right):
    return 2.0 * left * right / (left + right)


def pick(region, table):
    value = jnp.full(region.shape, table[0], F32)
    for idx in range(1, REGIONS):
        value = jnp.where(region == idx, table[idx], value)
    return value


def widen(compact):
    rows, count = compact.shape
    return jnp.concatenate([compact, jnp.zeros((rows, LANES - count), compact.dtype)], axis=1)


def spread(compact, index):
    return jnp.take_along_axis(compact, index, axis=1, mode="promise_in_bounds")


def kernel(
    nx, ny, rows, cols, cells,
    volt, drive, region, mask, sigma_hbm, cap_hbm, ws_hbm, wa_hbm,
    out, norms,
    sigma, cap, v, dr, reg, msk, ws, wa,
    halo_p, halo_n, reg_p, reg_n, col_l, col_r, con_l, con_r,
    x, s, y, nl, flux, side, turned, par, gain, plane, line, mine,
    sem_v, sem_d, sem_s, send_h, recv_h, send_c, recv_c, send_n, recv_n, hello,
):
    gx, gy = lax.axis_index("gx"), lax.axis_index("gy")
    up, down = lax.rem(gx + 1, nx), lax.rem(gx + nx - 1, nx)
    right, left = lax.rem(gy + 1, ny), lax.rem(gy + ny - 1, ny)
    groups = cols // 8

    small = [
        pltpu.make_async_copy(region, reg, sem_s.at[0]),
        pltpu.make_async_copy(mask, msk, sem_s.at[1]),
        pltpu.make_async_copy(ws_hbm, ws, sem_s.at[2]),
        pltpu.make_async_copy(wa_hbm, wa, sem_s.at[3]),
        pltpu.make_async_copy(sigma_hbm, sigma, sem_s.at[4]),
        pltpu.make_async_copy(cap_hbm, cap, sem_s.at[5]),
    ]
    for copy in small:
        copy.start()

    def load_row(r, c):
        for zt in range(ZT):
            pltpu.make_async_copy(
                volt.at[r, :, pl.ds(zt * LANES, LANES)],
                v.at[r, zt, pl.ds(PAD, cols), :],
                sem_v.at[r],
            ).start()
        pltpu.make_async_copy(drive.at[r], dr.at[r], sem_d.at[r]).start()
        return c

    lax.fori_loop(0, rows, load_row, 0)

    depth = nx // INNER
    gz, gi = gx // INNER, lax.rem(gx, INNER)
    base = gx - gi
    near_i = [gi] + [lax.rem(gi + i, INNER) for i in range(1, INNER)]
    near_y = [gy] + [lax.rem(gy + i, ny) for i in range(1, ny)]
    in_plane = [
        {"gx": base + near_i[i], "gy": near_y[k]} for k in range(ny) for i in range(INNER) if i or k
    ]
    in_line = [{"gx": lax.rem(gx + INNER * i, nx)} for i in range(1, depth)]

    def at(along, offset):
        mine_here, count = (gx, nx) if along == "gx" else (gy, ny)
        return {along: lax.rem(mine_here + offset + count, count)}

    beside = [at("gy", sign * i) for i in (1, 2) for sign in (1, -1)]
    near = [at("gx", sign * i) for i in range(1, INNER + 1) for sign in (1, -1)] + beside
    first = [at("gx", INNER), at("gx", -INNER)] + beside
    second = [at("gx", 2 * INNER), at("gx", -2 * INNER), at("gy", 2), at("gy", -2)]
    barrier = pltpu.get_barrier_semaphore()
    for where in near:
        pl.semaphore_signal(barrier, inc=1, device_id=where, device_id_type=MESH)

    def wait_volt(r):
        whole = v.at[r, :, pl.ds(PAD, cols), :]
        pltpu.make_async_copy(whole, whole, sem_v.at[r]).wait()

    def remote(src, dst, ssem, rsem, where):
        return pltpu.make_async_remote_copy(
            src_ref=src, dst_ref=dst, send_sem=ssem, recv_sem=rsem,
            device_id=where, device_id_type=MESH,
        )

    piece = cols // CHUNKS
    col_copies = [
        remote(volt.at[:, pl.ds(cols - 1, 1), :], col_l, send_c.at[0], recv_c.at[0], {"gy": right}),
        remote(par.at[:, 4, pl.ds(cols - 1, 1), :], con_l, send_c.at[1], recv_c.at[1], {"gy": right}),
        remote(volt.at[:, pl.ds(0, 1), :], col_r, send_c.at[2], recv_c.at[2], {"gy": left}),
        remote(par.at[:, 4, pl.ds(0, 1), :], con_r, send_c.at[3], recv_c.at[3], {"gy": left}),
    ]
    reg_copies = [
        remote(region.at[rows - 1], reg_p, send_h.at[0, CHUNKS], recv_h.at[0, CHUNKS], {"gx": up}),
        remote(region.at[0], reg_n, send_h.at[1, CHUNKS], recv_h.at[1, CHUNKS], {"gx": down}),
    ]
    row_copies = []
    for k in range(CHUNKS):
        part = pl.ds(k * piece, piece)
        row_copies.append((
            remote(volt.at[rows - 1, part, :], halo_p.at[part, :], send_h.at[0, k], recv_h.at[0, k], {"gx": up}),
            remote(volt.at[0, part, :], halo_n.at[part, :], send_h.at[1, k], recv_h.at[1, k], {"gx": down}),
        ))
    sends = reg_copies + col_copies + [copy for pair in row_copies for copy in pair]

    lane = lax.broadcasted_iota(jnp.int32, (8, LANES), 1)
    high = (lane >= KC).astype(jnp.int32)
    coef = lane % KC
    order = (coef % H + 1).astype(F32) * BASE_FREQ
    freq = jnp.where(coef < H, order, -order)
    partner = jnp.where(coef < H, lane + H, lane - H)
    own = [high + 2 * zt for zt in range(ZT)]
    within = [jnp.full((8, LANES), 2 * zt, jnp.int32) for zt in range(ZT)]
    across = [jnp.where(high == 0, 2 * zt - 1 if zt else NZ - 1, 2 * zt + 1) for zt in range(ZT)]
    left_half = lax.broadcasted_iota(jnp.int32, (cols, LANES), 1) < KC

    edge = jnp.zeros((PAD, LANES), F32)

    def clear(r, c):
        for zt in range(ZT):
            v[r, zt, pl.ds(0, PAD), :] = edge
            v[r, zt, pl.ds(cols + PAD, PAD), :] = edge
        return c

    lax.fori_loop(0, rows, clear, 0)
    flux[...] = jnp.zeros_like(flux)
    for zt in range(ZT):
        side[zt, pl.ds(0, PAD), :] = edge

    for copy in small:
        copy.wait()
    wait_volt(0)

    def pairs_of(r):
        for zt in range(ZT):
            value = v[r, zt, pl.ds(PAD, cols), :]
            other = pltpu.roll(value, KC, 1)
            rest = value - value.astype(BF16).astype(F32)
            other_rest = other - other.astype(BF16).astype(F32)
            x[pl.ds(zt * cols, cols), :] = jnp.where(left_half, value, other_rest).astype(BF16)
            x[pl.ds((ZT + zt) * cols, cols), :] = jnp.where(left_half, other, rest).astype(BF16)
            turned[zt] = other

    pairs_of(0)

    pairs = rows // 2
    pair_lane = lax.broadcasted_iota(jnp.int32, (NZ, LANES), 1)
    layer = lax.broadcasted_iota(jnp.int32, (NZ, LANES), 0)
    pair_regions = [jnp.concatenate([reg[2 * p], reg[2 * p + 1]], axis=1) for p in range(pairs)]
    conduct = [pick(both, sigma) for both in pair_regions]
    for p in range(pairs):
        here = conduct[p]
        beyond = pltpu.roll(conduct[p + 1], cols, 1) if p + 1 < pairs else jnp.zeros_like(here)
        there = jnp.where(pair_lane < cols, pltpu.roll(here, cols, 1), beyond)
        after = jnp.where(pair_lane % cols == cols - 1, 0.0, pltpu.roll(here, LANES - 1, 1))
        deeper = jnp.where(layer == NZ - 1, 0.0, pltpu.roll(here, NZ - 1, 0))
        diode = jnp.concatenate([msk[2 * p], msk[2 * p + 1]], axis=1)
        held_charge = pick(pair_regions[p], cap)
        fields = (
            harmonic_mean(here, there), harmonic_mean(here, after), harmonic_mean(here, deeper),
            jnp.where(diode != 0, -held_charge, held_charge), here,
        )
        for i, field in enumerate(fields):
            flat = widen(jnp.transpose(field))
            par[2 * p, i] = flat[:cols]
            par[2 * p + 1, i] = flat[cols:]

    def linear(r):
        after = jnp.minimum(r + 1, rows - 1)
        for zt in range(ZT):
            lanes = pl.ds(zt * LANES, LANES)

            def gains(i, index):
                return [spread(par[r, i, pl.ds(8 * j, 8), :], index) for j in range(groups)]

            g_row, g_next, charge = gains(0, own[zt]), gains(1, own[zt]), gains(3, own[zt])
            g_in, g_out = gains(2, within[zt]), gains(2, across[zt])
            for j in range(groups):
                spot = pl.ds(8 * j, 8)
                value = v[r, zt, pl.ds(PAD + 8 * j, 8), :]
                flow = g_row[j] * (value - v[after, zt, pl.ds(PAD + 8 * j, 8), :])
                total = flow - flux[spot, lanes] - dr[r, spot, lanes]
                flux[spot, lanes] = flow
                flow = g_next[j] * (value - v[r, zt, pl.ds(PAD + 8 * j + 1, 8), :])
                side[zt, pl.ds(PAD + 8 * j, 8), :] = flow
                total += flow - side[zt, pl.ds(PAD + 8 * j - 1, 8), :]
                total += g_in[j] * (value - turned[zt, spot, :])
                outer = jnp.where(high == 0, turned[max(zt - 1, 0), spot, :], turned[min(zt + 1, ZT - 1), spot, :])
                total += g_out[j] * (value - outer)
                total += jnp.abs(charge[j]) * (freq * spread(value, partner))
                total += jnp.where(charge[j] < 0.0, 0.5 * value + nl[pl.ds(zt * cols + 8 * j, 8), :], 0.0)
                out[r, spot, lanes] = total


    def one_row(r, c):
        @pl.when(r == SEND_AT)
        def _():
            pl.semaphore_wait(barrier, len(near))
            for copy in sends:
                copy.start()
            for where in first:
                pl.semaphore_signal(hello.at[0], inc=1, device_id=where, device_id_type=MESH)

        @pl.when(r == rows // 2)
        def _():
            pl.semaphore_wait(hello.at[0], len(first))
            for where in second:
                pl.semaphore_signal(hello.at[1], inc=1, device_id=where, device_id_type=MESH)

        @pl.when(r < rows - 1)
        def _():
            wait_volt(r + 1)

        pltpu.make_async_copy(dr.at[r], dr.at[r], sem_d.at[r]).wait()
        xs = x[...]
        s[...] = jnp.dot(jnp.concatenate([xs, xs], axis=1), ws[...], preferred_element_type=F32)
        for zt in range(ZT):
            for half in range(2):
                wave = s[pl.ds((half * ZT + zt) * cols, cols), :]
                bent = jnp.tanh(wave)
                soft = jnp.abs(wave) - jnp.log(1.0 + jnp.abs(bent))
                y[pl.ds(zt * cols, cols), pl.ds(half * 2 * S, S)] = soft.astype(BF16)
                y[pl.ds(zt * cols, cols), pl.ds(half * 2 * S + S, S)] = bent.astype(BF16)
        full = jnp.dot(y[...], wa[...], preferred_element_type=F32)
        nl[...] = full[:, :LANES] + full[:, LANES:]
        linear(r)
        pairs_of(jnp.minimum(r + 1, rows - 1))
        return c

    lax.fori_loop(0, rows, one_row, 0)

    for copy in col_copies:
        copy.wait_recv()
    sub = lax.broadcasted_iota(jnp.int32, (8, LANES), 0)

    def fix_cols(r, acc):
        first = par[r, 4, pl.ds(0, 8), :]
        last = par[r, 4, pl.ds(cols - 8, 8), :]
        before = jnp.broadcast_to(con_l[r], (8, LANES))
        behind = jnp.broadcast_to(con_r[r], (8, LANES))
        g_l = jnp.where((sub == 0) & (lane < NZ) & (gy > 0), harmonic_mean(first, before), 0.0)
        g_r = jnp.where((sub == 7) & (lane < NZ) & (gy < ny - 1), harmonic_mean(last, behind), 0.0)
        for zt in range(ZT):
            lanes = pl.ds(zt * LANES, LANES)
            out[r, pl.ds(0, 8), lanes] += spread(g_l, own[zt]) * (
                v[r, zt, pl.ds(PAD, 8), :] - jnp.broadcast_to(col_l[r, :, lanes], (8, LANES))
            )
            out[r, pl.ds(cols - 8, 8), lanes] += spread(g_r, own[zt]) * (
                v[r, zt, pl.ds(PAD + cols - 8, 8), :] - jnp.broadcast_to(col_r[r, :, lanes], (8, LANES))
            )
        inner = jnp.where((r > 0) & (r < rows - 1), 1.0, 0.0)
        parts = [jnp.zeros((8, LANES), F32) for _ in range(8)]
        for zt in range(ZT):
            for j in range(groups):
                value = out[r, pl.ds(8 * j, 8), pl.ds(zt * LANES, LANES)]
                parts[j % 8] = parts[j % 8] + value * value
        while len(parts) > 1:
            parts = [a + b for a, b in zip(parts[::2], parts[1::2])]
        return acc + inner * parts[0]

    def fix_some(p, acc):
        for i in range(4):
            acc = fix_cols(4 * p + i, acc)
        return acc

    acc = lax.fori_loop(0, rows // 4, fix_some, jnp.zeros((8, LANES), F32))

    for end, (copy, marks, r) in enumerate(zip(reg_copies, (reg_p, reg_n), (0, rows - 1))):
        copy.wait_recv()
        field = jnp.concatenate([pick(marks[...], sigma), jnp.zeros((NZ, LANES - cols), F32)], axis=1)
        flat = widen(jnp.transpose(field))[:cols]
        inside = lax.broadcasted_iota(jnp.int32, (cols, LANES), 1) < NZ
        gain[end] = jnp.where(inside, harmonic_mean(par[r, 4], flat), 0.0)
    for k in range(CHUNKS):
        for end, (copy, halo, r) in enumerate(zip(row_copies[k], (halo_p, halo_n), (0, rows - 1))):
            copy.wait_recv()
            parts = [jnp.zeros((8, LANES), F32) for _ in range(8)]
            for j in range(k * piece // 8, (k + 1) * piece // 8):
                spot = pl.ds(8 * j, 8)
                for zt in range(ZT):
                    lanes = pl.ds(zt * LANES, LANES)
                    value = out[r, spot, lanes] + spread(gain[end, spot, :], own[zt]) * (
                        v[r, zt, pl.ds(8 * j + PAD, 8), :] - halo[spot, lanes]
                    )
                    out[r, spot, lanes] = value
                    parts[zt % 8] = parts[zt % 8] + value * value
            while len(parts) > 1:
                parts = [a + b for a, b in zip(parts[::2], parts[1::2])]
            acc = acc + parts[0]

    local = jnp.sum(acc, axis=0, keepdims=True)
    pl.semaphore_wait(hello.at[1], len(second))

    def reduce_over(others, here, value, buf, slot):
        mine[slot] = value
        spot = buf.at[pl.ds(here, 1), :]
        buf[pl.ds(here, 1), :] = value
        for where in others:
            remote(mine.at[slot], spot, send_n.at[slot], recv_n.at[slot], where).start()
        rest = buf.at[pl.ds(0, len(others)), :]
        pltpu.make_async_copy(rest, rest, recv_n.at[slot]).wait()
        return jnp.sum(buf[...], axis=0, keepdims=True)

    value = local + pltpu.roll(local, KC, 1)
    value = reduce_over(in_plane, gy * INNER + gi, value, plane, 0)
    value = reduce_over(in_line, gz, value, line, 1)
    norms[...] = jnp.sqrt(value / cells + NORM_EPS)[0, :KC]

    for slot, buf in enumerate((plane, line)):
        others = buf.at[pl.ds(0, buf.shape[0] - 1), :]
        pltpu.make_async_copy(others, others, send_n.at[slot]).wait()
    for copy in sends:
        copy.wait_send()


def write_out(residual, norms, residual_out, norms_out, sems):
    count = residual.shape[0]
    copies = [pltpu.make_async_copy(residual.at[r], residual_out.at[r], sems.at[r]) for r in range(count)]
    copies.append(pltpu.make_async_copy(norms, norms_out, sems.at[count]))
    for copy in copies:
        copy.start()
    for copy in copies:
        copy.wait()


def body(nx, ny, volt, drive, region, diode_mask, sigma_table, cap_table):
    rows, cols, width = volt.shape
    cells = rows * cols * NZ * nx * ny
    ws, wa = spectral_tables()
    hbm = pl.BlockSpec(memory_space=pltpu.HBM)
    vmem = pl.BlockSpec(memory_space=pltpu.VMEM)
    dma = pltpu.SemaphoreType.DMA
    held = functools.partial(pltpu.with_memory_space_constraint, memory_space=pltpu.HBM)
    residual, norms = pl.pallas_call(
        functools.partial(kernel, nx, ny, rows, cols, cells),
        out_shape=(
            jax.ShapeDtypeStruct((rows, cols, width), F32),
            jax.ShapeDtypeStruct((KC,), F32),
        ),
        in_specs=[hbm] * 8,
        out_specs=(vmem, vmem),
        scratch_shapes=[
            pltpu.SMEM((REGIONS,), F32),
            pltpu.SMEM((REGIONS,), F32),
            pltpu.VMEM((rows, ZT, cols + 2 * PAD, LANES), F32),
            pltpu.VMEM((rows, cols, width), F32),
            pltpu.VMEM((rows, NZ, cols), jnp.int32),
            pltpu.VMEM((rows, NZ, cols), jnp.int32),
            pltpu.VMEM(ws.shape, BF16),
            pltpu.VMEM(wa.shape, BF16),
            pltpu.VMEM((cols, width), F32),
            pltpu.VMEM((cols, width), F32),
            pltpu.VMEM((NZ, cols), jnp.int32),
            pltpu.VMEM((NZ, cols), jnp.int32),
            pltpu.VMEM((rows, 1, width), F32),
            pltpu.VMEM((rows, 1, width), F32),
            pltpu.VMEM((rows, 1, LANES), F32),
            pltpu.VMEM((rows, 1, LANES), F32),
            pltpu.VMEM((2 * ZT * cols, LANES), BF16),
            pltpu.VMEM((2 * ZT * cols, S), F32),
            pltpu.VMEM((ZT * cols, 4 * S), BF16),
            pltpu.VMEM((ZT * cols, LANES), F32),
            pltpu.VMEM((cols, width), F32),
            pltpu.VMEM((ZT, cols + PAD, LANES), F32),
            pltpu.VMEM((ZT, cols, LANES), F32),
            pltpu.VMEM((rows, 5, cols, LANES), F32),
            pltpu.VMEM((2, cols, LANES), F32),
            pltpu.VMEM((ny * INNER, LANES), F32),
            pltpu.VMEM((nx // INNER, LANES), F32),
            pltpu.VMEM((2, 1, LANES), F32),
            dma((rows,)), dma((rows,)), dma((6,)),
            dma((2, CHUNKS + 1)), dma((2, CHUNKS + 1)),
            dma((4,)), dma((4,)),
            dma((2,)), dma((2,)), pltpu.SemaphoreType.REGULAR((2,)),
        ],
        compiler_params=pltpu.CompilerParams(
            collective_id=0, has_side_effects=True, vmem_limit_bytes=38 * 1024 * 1024
        ),
        name="residual",
    )(
        held(volt), held(drive), held(jnp.swapaxes(region, 1, 2)), held(jnp.swapaxes(diode_mask, 1, 2)),
        held(sigma_table), held(cap_table), held(ws), held(wa),
    )
    return pl.pallas_call(
        write_out,
        out_shape=(jax.ShapeDtypeStruct(residual.shape, F32), jax.ShapeDtypeStruct(norms.shape, F32)),
        in_specs=[vmem, vmem],
        out_specs=(hbm, hbm),
        scratch_shapes=[dma((rows + 1,))],
        compiler_params=pltpu.CompilerParams(vmem_limit_bytes=8 * 1024 * 1024),
        name="write_out",
    )(residual, norms)


def solution(mesh):
    nx, ny = mesh.shape["gx"], mesh.shape["gy"]
    cut = P("gx", "gy", None)
    return jax.shard_map(
        functools.partial(body, nx, ny), mesh=mesh, in_specs=(cut, cut, cut, cut, P(), P()),
        out_specs=(cut, P()), check_vma=False,
    )
```
